256 devices in a mesh: tm: 32 (over z, x_lo, core), grp: 8 (over y, x_hi).
Axes of the slice: x: 4 (x_hi: 2, x_lo: 2; x = x_hi * 2 + x_lo), y: 4, z: 8, core: 2. Of those that a mesh axis runs over, the one named last changes fastest.
Arguments:
- residual: float32 [32, 8, 3072], P('tm', 'grp'), may hold values from -6 to 6
- weight: float32 [32, 8, 3072], P('tm', 'grp'), may hold values from 0.25 to 4
- source_part: float32 [5, 32, 8, 3072], P(None, 'tm', 'grp'), may hold values from -2.5 to 2.5
- source_index: int32 [32, 8, 3072], P('tm', 'grp'), may hold values from 0 to 4095
- source_delta: float32 [5, 32, 4096], P(None, 'tm'), may hold values from -6 to 6
- attitude_part: float32 [3, 32, 8, 3072], P(None, 'tm', 'grp'), may hold values from -6 to 6
- spline_phase: float32 [32, 8, 3072], P('tm', 'grp'), may hold values from 0 to 1
- knot_index: int32 [32, 8, 3072], P('tm', 'grp'), may hold values from 0 to 3071, as said below
- calib_part: float32 [6, 32, 8, 3072], P(None, 'tm', 'grp'), may hold values from -6 to 6
- calib_index: int32 [32, 8, 3072], P('tm', 'grp'), may hold values from 0 to 2047
- global_part: float32 [4, 32, 8, 3072], P(None, 'tm', 'grp'), may hold values from -6 to 6
Outputs:
- residual_new: float32 [32, 8, 3072], P('tm', 'grp')
- attitude_step: float32 [3, 3072], P(None, 'tm')
- calib_step: float32 [6, 2048], replicated
- global_step: float32 [4], replicated
The draws below stay inside these ranges and needn't reach their ends.
Inputs may be any that keep to these rules, and one draw needn't show every extreme that they name: `knot_index`: observation r of interval t (in any group) lies in knot interval t * 96 + 4 * (r // 128) + j for some j in 0 .. 3.
All inputs are finite; a program needn't handle non-finite values.
Results may differ from the reference program's by a relative error of at most 0.00012.
Values sent between devices are 32-bit elements; how exact they have to be, the bound alone decides.
No kernel may reach another device: no remote copies, remote signals or barrier semaphores. Data moves between devices by JAX's collectives and lax.ppermute only.
A program may use at most 128 MiB of HBM per device.

```python
import math
import jax
import jax.numpy as jnp
from jax import lax

ROWS_DEV = 3072
TILE = 128
KPT = 4
SRC_DEV = 4096
UNITS = 2048
CPAR = 6
GPAR = 4
ATT_SWEEPS = 4
ND = 96
INTERVALS = 32
GROUPS = 8


def draw_knot_index(key, part):
    within = jax.random.randint(key, (INTERVALS, GROUPS, ROWS_DEV), 0, KPT, dtype=jnp.int32)
    tile_base = KPT * (jnp.arange(ROWS_DEV, dtype=jnp.int32) // TILE)
    interval_base = jnp.arange(INTERVALS, dtype=jnp.int32) * ND
    return (interval_base[:, None, None] + tile_base[None, None, :] + within).astype(jnp.int32)


def with_ends(drawn, rng, low, top_value):
    longest = drawn.shape.index(max(drawn.shape))
    spots = []
    for shift in (0, 1):
        where = [jax.random.randint(jax.random.fold_in(rng, axis), (), 0, length) for axis, length in enumerate(drawn.shape)]
        where[longest] = (where[longest] + shift) % drawn.shape[longest]
        spots.append(tuple(where))
    return drawn.at[spots[0]].set(low).at[spots[1]].set(top_value)


def level_of(stream_key, shape, cuts, least, top_value):
    loudness, own = 1.0, jax.random.fold_in(stream_key, 6)
    for dim, parts in cuts:
        steps = jnp.exp(jax.random.uniform(jax.random.fold_in(own, dim), (parts,), jnp.float32, least / len(cuts), top_value / len(cuts)))
        loudness = loudness * jnp.repeat(steps, shape[dim] // parts).reshape([-1 if axis == dim else 1 for axis in range(len(shape))])
    return loudness


def scatter_about(own_key, dims, scale, limit, split=(), kind=jnp.bfloat16):
    array = scale * jax.random.normal(own_key, dims, jnp.float32)
    if split:
        array = array * level_of(own_key, dims, split, -0.22, 0.18)
    return jnp.clip(array, -limit, limit).astype(kind)


def setup_inputs(seed: int = 0) -> dict:
    streams_of = jax.random.split(jax.random.key(seed), 12)
    return {
        "residual": scatter_about(streams_of[0], (INTERVALS, GROUPS, ROWS_DEV), 1.0, 6.0, ((0, 32), (1, 8)), jnp.float32),
        "weight": jnp.clip(jnp.exp(math.log(4.0) - 2.7725887 * jax.random.uniform(streams_of[1], (INTERVALS, GROUPS, ROWS_DEV), jnp.float32) ** level_of(streams_of[1], (INTERVALS, GROUPS, ROWS_DEV), ((0, 32), (1, 8)), -0.2, 0.2)), 0.25, 4.0),
        "source_part": scatter_about(streams_of[2], (5, INTERVALS, GROUPS, ROWS_DEV), 5 ** -0.5, 2.5, ((1, 32), (2, 8)), jnp.float32),
        "source_index": with_ends(jax.random.randint(streams_of[3], (INTERVALS, GROUPS, ROWS_DEV), 0, SRC_DEV), jax.random.fold_in(streams_of[3], 1), 0, SRC_DEV - 1).astype(jnp.int32),
        "source_delta": scatter_about(streams_of[4], (5, INTERVALS, SRC_DEV), 1.0, 6.0, ((1, 32),), jnp.float32),
        "attitude_part": scatter_about(streams_of[5], (3, INTERVALS, GROUPS, ROWS_DEV), 1.0, 6.0, ((1, 32), (2, 8)), jnp.float32),
        "spline_phase": jnp.clip(1.0 * jax.random.uniform(streams_of[6], (INTERVALS, GROUPS, ROWS_DEV), jnp.float32) ** level_of(streams_of[6], (INTERVALS, GROUPS, ROWS_DEV), ((0, 32), (1, 8)), -0.2, 0.2), 0.0, 1.0),
        "knot_index": draw_knot_index(jax.random.fold_in(streams_of[11], 71), 0),
        "calib_part": scatter_about(streams_of[8], (CPAR, INTERVALS, GROUPS, ROWS_DEV), 1.0, 6.0, ((1, 32), (2, 8)), jnp.float32),
        "calib_index": with_ends(jax.random.randint(streams_of[9], (INTERVALS, GROUPS, ROWS_DEV), 0, UNITS), jax.random.fold_in(streams_of[9], 1), 0, UNITS - 1).astype(jnp.int32),
        "global_part": scatter_about(streams_of[10], (GPAR, INTERVALS, GROUPS, ROWS_DEV), 1.0, 6.0, ((1, 32), (2, 8)), jnp.float32),
    }


OMEGA = 0.6
RIDGE = 1.0

def spline_basis(phase):
    inverse = 1.0 - phase
    square = phase * phase
    cubed = square * phase
    return [inverse * inverse * inverse / 6.0, (3.0 * cubed - 6.0 * square + 4.0) / 6.0, (-3.0 * cubed + 3.0 * square + 3.0 * phase + 1.0) / 6.0, cubed / 6.0]

def cholesky_lists(matrix, extent):
    lower_tri = [[None for column in range(extent)] for target in range(extent)]
    for column in range(extent):
        pivot_sq = matrix[column][column]
        for inner_k in range(column):
            pivot_sq = pivot_sq - lower_tri[column][inner_k] * lower_tri[column][inner_k]
        pivot_val = jnp.sqrt(pivot_sq)
        lower_tri[column][column] = pivot_val
        for target in range(column + 1, extent):
            entry_val = matrix[target][column]
            for inner_k in range(column):
                entry_val = entry_val - lower_tri[target][inner_k] * lower_tri[column][inner_k]
            lower_tri[target][column] = entry_val / pivot_val
    return lower_tri

def solve_lower(lower_tri, vector):
    result = []
    for target in range(len(vector)):
        running = vector[target]
        for inner_k in range(target):
            running = running - lower_tri[target][inner_k] * result[inner_k]
        result.append(running / lower_tri[target][target])
    return result

def solve_upper(lower_tri, vector):
    extent = len(vector)
    result = [None for target in range(extent)]
    for target in reversed(range(extent)):
        running = vector[target]
        for inner_k in range(target + 1, extent):
            running = running - lower_tri[inner_k][target] * result[inner_k]
        result[target] = running / lower_tri[target][target]
    return result

def upper_pairs(extent):
    return [(first, second) for first in range(extent) for second in range(first, extent)]

def symmetric_lists(upper_values, extent):
    matrix = [[None for second in range(extent)] for first in range(extent)]
    for position, index_pair in enumerate(upper_pairs(extent)):
        first, second = index_pair
        value_now = upper_values[position] + (RIDGE if first == second else 0.0)
        matrix[first][second] = value_now
        matrix[second][first] = value_now
    return matrix

def solve_blocks(upper_values, rhs_values, extent):
    lower_tri = cholesky_lists(symmetric_lists(upper_values, extent), extent)
    whitened = solve_lower(lower_tri, rhs_values)
    solution = solve_upper(lower_tri, whitened)
    return (jnp.stack(whitened), jnp.stack(solution))

def apply_band(band_own, band_left, padded):
    extent = band_own.shape[-1]
    result = padded[:, 3:3 + extent]
    for offset in range(4):
        ahead_x = padded[:, 3 + offset:3 + offset + extent]
        result = result + lax.optimization_barrier(jnp.sum(band_own[offset] * ahead_x[None, :, :], axis=1))
    for offset in range(1, 4):
        behind = padded[:, 3 - offset:3 - offset + extent]
        blocks = band_left[offset][:, :, 3 - offset:3 - offset + extent]
        result = result + lax.optimization_barrier(jnp.sum(blocks * behind[:, None, :], axis=0))
    return result

def node_sweeps(band_own, band_left, rhs_att, extend):
    diagonal = [[band_own[0][first, second] + (RIDGE if first == second else 0.0) for second in range(3)] for first in range(3)]
    lower_tri = cholesky_lists(diagonal, 3)

    def precondition(vector):
        return jnp.stack(solve_upper(lower_tri, solve_lower(lower_tri, [vector[axis_k] for axis_k in range(3)])))
    answer = OMEGA * precondition(rhs_att)
    for sweep_no in range(1, ATT_SWEEPS):
        padded = extend(answer)
        answer = answer + OMEGA * precondition(rhs_att - apply_band(band_own, band_left, padded))
    padded = extend(answer)
    scaled = jnp.stack([sum((lower_tri[inner_k][target] * answer[inner_k] for inner_k in range(target, 3))) for target in range(3)])
    return (answer, padded, scaled)

def node_features(vectors, weights, first_res, basis_no):
    term_list = []
    for offset in range(4 - basis_no):
        for first in range(3):
            for second in range(3):
                term_list.append(weights * vectors[basis_no][first] * vectors[basis_no + offset][second])
    for first in range(3):
        term_list.append(weights * vectors[basis_no][first] * first_res)
    return jnp.stack(term_list)

def spread_terms(stacked, basis_no):
    band_rows = (4 - basis_no) * 9
    filler = jnp.zeros((basis_no * 9,) + stacked.shape[1:], jnp.float32)
    return jnp.concatenate([stacked[:band_rows], filler, stacked[band_rows:]], axis=0)

def unit_matrix_terms(rows_part, weights):
    return [weights * rows_part[first] * rows_part[second] for first, second in upper_pairs(rows_part.shape[0])]

def rhs_terms(rows_part, weights, resid_now):
    return [weights * rows_part[first] * resid_now for first in range(rows_part.shape[0])]

def reference(residual, weight, source_part, source_index, source_delta, attitude_part, spline_phase, knot_index, calib_part, calib_index, global_part):
    nodes_dev = ND
    interval_ids = jnp.arange(INTERVALS, dtype=jnp.int32)

    def interval_rows(index_t):
        weights = weight[index_t].reshape(-1)
        source_rows = source_part[:, index_t].reshape(5, -1)
        picked = jnp.take(source_delta[:, index_t], source_index[index_t].reshape(-1), axis=1)
        first_res = residual[index_t].reshape(-1) - lax.optimization_barrier(jnp.sum(source_rows * picked, axis=0))
        basis_list = spline_basis(spline_phase[index_t].reshape(-1))
        att_rows = attitude_part[:, index_t].reshape(3, -1)
        vectors = [basis_val[None, :] * att_rows for basis_val in basis_list]
        local_knot = knot_index[index_t].reshape(-1) - index_t * nodes_dev
        return (weights, first_res, vectors, local_knot)

    def first_pass(index_t):
        weights, first_res, vectors, local_knot = interval_rows(index_t)
        local_sums = jnp.zeros((39, nodes_dev + 3), jnp.float32)
        for basis_no in range(4):
            stacked = node_features(vectors, weights, first_res, basis_no)
            binned = jax.ops.segment_sum(stacked.T, local_knot + basis_no, num_segments=nodes_dev + 3).T
            local_sums = local_sums + spread_terms(binned, basis_no)
        return local_sums
    local_all = lax.map(first_pass, interval_ids)
    spill_out = local_all[:, :, nodes_dev:]
    shifted = jnp.concatenate([jnp.zeros((1, 39, 3), jnp.float32), spill_out[:-1]], axis=0)
    main_part = local_all[:, :, :nodes_dev]
    main_part = jnp.concatenate([main_part[:, :, :3] + shifted, main_part[:, :, 3:]], axis=2)
    totals = jnp.transpose(main_part, (1, 0, 2)).reshape(39, INTERVALS * nodes_dev)
    band_own = totals[:36].reshape(4, 3, 3, -1)
    band_left = jnp.concatenate([jnp.zeros((4, 3, 3, 3), jnp.float32), band_own], axis=3)

    def extend(vector):
        return jnp.pad(vector, ((0, 0), (3, 3)))
    answer, padded, attitude_step = node_sweeps(band_own, band_left, totals[36:], extend)
    node_values = padded[:, 3:]

    def second_pass(index_t):
        weights, first_res, vectors, local_knot = interval_rows(index_t)
        global_knot = knot_index[index_t].reshape(-1)
        second_res = first_res
        for basis_no in range(4):
            picked_nodes = jnp.take(node_values, global_knot + basis_no, axis=1)
            second_res = second_res - lax.optimization_barrier(jnp.sum(vectors[basis_no] * picked_nodes, axis=0))
        calib_rows = calib_part[:, index_t].reshape(CPAR, -1)
        global_rows = global_part[:, index_t].reshape(GPAR, -1)
        unit_ids = calib_index[index_t].reshape(-1)
        features = jnp.stack(unit_matrix_terms(calib_rows, weights) + rhs_terms(calib_rows, weights, second_res))
        unit_terms = jax.ops.segment_sum(features.T, unit_ids, num_segments=UNITS).T
        global_terms = jnp.stack([jnp.sum(term_row) for term_row in unit_matrix_terms(global_rows, weights) + rhs_terms(global_rows, weights, second_res)])
        return (second_res, unit_terms, global_terms)
    second_all, unit_all, global_all = lax.map(second_pass, interval_ids)
    unit_total = lax.optimization_barrier(jnp.sum(unit_all, axis=0))
    global_total = lax.optimization_barrier(jnp.sum(global_all, axis=0))
    pair_count = CPAR * (CPAR + 1) // 2
    pair_global = GPAR * (GPAR + 1) // 2
    calib_step, calib_solution = solve_blocks(unit_total[:pair_count], [unit_total[pair_count + first] for first in range(CPAR)], CPAR)
    global_step, global_solution = solve_blocks(global_total[:pair_global], [global_total[pair_global + first] for first in range(GPAR)], GPAR)

    def third_pass(carried):
        index_t, second_res = carried
        calib_rows = calib_part[:, index_t].reshape(CPAR, -1)
        global_rows = global_part[:, index_t].reshape(GPAR, -1)
        unit_values = jnp.take(calib_solution, calib_index[index_t].reshape(-1), axis=1)
        final_res = second_res - lax.optimization_barrier(jnp.sum(calib_rows * unit_values, axis=0)) - lax.optimization_barrier(jnp.sum(global_rows * global_solution[:, None], axis=0))
        return final_res.reshape(GROUPS, ROWS_DEV)
    residual_new = lax.map(third_pass, (interval_ids, second_all))
    return (residual_new, attitude_step, calib_step, global_step)
```

```python
import jax
import jax.numpy as jnp
from jax import lax
from jax.experimental import pallas as pl
from jax.experimental.pallas import tpu as pltpu
from jax.sharding import PartitionSpec as P

LANES = 128
TILES = 24
KPT = 4
UNITS = 2048
CPAR = 6
GPAR = 4
SPAR = 5
ATT_SWEEPS = 4
ND = 96
HALO = 9
OMEGA = 0.6
RIDGE = 1.0
HI = 8
LO = 256
BASES = (27, 21, 15, 9)
F32 = jnp.float32
BF16 = jnp.bfloat16


def pairs(extent):
    return [(a, b) for a in range(extent) for b in range(a, extent)]


PAIR_AT = {extent: {p: i for i, p in enumerate(pairs(extent))} for extent in (3, 4, 6)}


def entry(values, extent, a, b):
    return values[PAIR_AT[extent][(min(a, b), max(a, b))]]


def factor(values, extent):
    low = [[None] * extent for _ in range(extent)]
    inv = [None] * extent
    for c in range(extent):
        pivot = entry(values, extent, c, c) + RIDGE
        for k in range(c):
            pivot = pivot - low[c][k] * low[c][k]
        low[c][c] = jnp.sqrt(pivot)
        inv[c] = 1.0 / low[c][c]
        for r in range(c + 1, extent):
            value = entry(values, extent, r, c)
            for k in range(c):
                value = value - low[r][k] * low[c][k]
            low[r][c] = value * inv[c]
    return low, inv


def forward(low, inv, vector):
    out = []
    for r in range(len(vector)):
        value = vector[r]
        for k in range(r):
            value = value - low[r][k] * out[k]
        out.append(value * inv[r])
    return out


def backward(low, inv, vector):
    extent = len(vector)
    out = [None] * extent
    for r in reversed(range(extent)):
        value = vector[r]
        for k in range(r + 1, extent):
            value = value - low[k][r] * out[k]
        out[r] = value * inv[r]
    return out


def spline(u):
    v = 1.0 - u
    s = u * u
    c = s * u
    sixth = 1.0 / 6.0
    return [
        v * v * v * sixth,
        (3.0 * c - 6.0 * s + 4.0) * sixth,
        (-3.0 * c + 3.0 * s + 3.0 * u + 1.0) * sixth,
        c * sixth,
    ]


def halves(x):
    top = x.astype(BF16).astype(F32)
    return top, x - top


def dot_nt(a, b):
    return lax.dot_general(a, b, (((1,), (1,)), ((), ())), preferred_element_type=F32)


def attitude_kernel(res, w, sp, si, sd, ap, ph, kn, first_out, att_out, feat, lhs, hot, acc):
    index = si[...]
    row_id = index >> 7
    lane_id = index & (LANES - 1)
    picked = [jnp.zeros((TILES, LANES), F32) for _ in range(SPAR)]
    for h in range(sd.shape[1]):
        mine = row_id == h
        for c in range(SPAR):
            row = jnp.broadcast_to(sd[c, h : h + 1, :], (TILES, LANES))
            picked[c] = jnp.where(mine, jnp.take_along_axis(row, lane_id, axis=1), picked[c])
    total = sp[0] * picked[0]
    for c in range(1, SPAR):
        total = total + sp[c] * picked[c]
    first = res[...] - total
    first_out[...] = first
    basis = spline(ph[...])
    weight = w[...]
    att = [ap[a] for a in range(3)]
    outer = [weight * att[a] * att[b] for a, b in pairs(3)]
    right = [weight * att[a] * first for a in range(3)]
    at = 0
    for i in range(4):
        for value in right:
            feat[pl.ds(at * TILES, TILES), :] = basis[i] * value
            at += 1
        for d in range(4 - i):
            both = basis[i] * basis[i + d]
            for value in outer:
                feat[pl.ds(at * TILES, TILES), :] = both * value
                at += 1
    count = at
    padded = lhs.shape[0] // 2
    node = lax.broadcasted_iota(jnp.int32, (LANES, LANES), 0)
    for t in range(TILES):
        cols = slice(t * LANES, (t + 1) * LANES)
        top, low = halves(feat[pl.ds(t, count, stride=TILES), :])
        lhs[0:count, cols] = top.astype(BF16)
        lhs[padded : padded + count, cols] = low.astype(BF16)
        slot = (kn[t : t + 1, :] & (KPT - 1)) + (KPT * t + HALO)
        hot[:, cols] = jnp.where(node == slot, 1.0, 0.0).astype(BF16)
    both = dot_nt(lhs[...], hot[...])
    acc[...] = both[:padded] + both[padded:]
    att_out[...] = jnp.zeros_like(att_out)
    at = 0
    for i, rows in enumerate(BASES):
        value = acc[at : at + rows, :]
        if i:
            value = pltpu.roll(value, i, 1)
        att_out[0:rows, :] = att_out[0:rows, :] + value
        at += rows


def unit_hot(unit, hot):
    lo_id = lax.broadcasted_iota(jnp.int32, (LO, LANES), 0)
    for t in range(TILES):
        cols = slice(t * LANES, (t + 1) * LANES)
        lo = unit[t : t + 1, :] & (LO - 1)
        hot[:, cols] = jnp.where(lo_id == lo, 1.0, 0.0).astype(BF16)


def spread(unit, feats, parts, base, top_to, low_to):
    for f, value in enumerate(feats):
        top, low = halves(value)
        parts[0, pl.ds(f * TILES, TILES), :] = top
        parts[1, pl.ds(f * TILES, TILES), :] = low
    hi_id = lax.broadcasted_iota(jnp.int32, (HI, LANES), 0)
    zero = jnp.zeros((HI, LANES), F32)
    for t in range(TILES):
        cols = slice(t * LANES, (t + 1) * LANES)
        mine = hi_id == (unit[t : t + 1, :] >> 8)
        for part, to in ((0, top_to), (1, low_to)):
            for f in range(0, len(feats), 2):
                rows = []
                for g in (f, f + 1):
                    if g < len(feats):
                        row = parts[part, g * TILES + t : g * TILES + t + 1, :]
                        rows.append(jnp.where(mine, jnp.broadcast_to(row, (HI, LANES)), 0.0))
                    else:
                        rows.append(zero)
                to[base + f * HI : base + (f + 2) * HI, cols] = jnp.concatenate(rows, axis=0).astype(BF16)


def totals_row(values, first_lane):
    lane = lax.broadcasted_iota(jnp.int32, (1, LANES), 1)
    row = jnp.zeros((1, LANES), F32)
    for k, value in enumerate(values):
        folded = value[0:8] + value[8:16] + value[16:24]
        total = jnp.sum(jnp.sum(folded, axis=1, keepdims=True), axis=0, keepdims=True)
        row = jnp.where(lane == first_lane + k, total, row)
    return row


N_C = CPAR * (CPAR + 1) // 2
N_G = GPAR * (GPAR + 1) // 2
E_COL = N_C * HI - LANES
G_COL = E_COL + CPAR * HI
H_COL = G_COL + N_G


def matrix_kernel(w, cp, ci, gp, left_out, right_out, hot_out, parts, top, low):
    weight = w[...]
    calib = [cp[a] for a in range(CPAR)]
    weighted = [weight * c for c in calib]
    feats = [weighted[a] * calib[b] for a, b in pairs(CPAR)]
    used = (N_C + 1) // 2 * 2 * HI
    top[used:, :] = jnp.zeros((2 * LANES - used, top.shape[1]), BF16)
    low[used:, :] = jnp.zeros((2 * LANES - used, top.shape[1]), BF16)
    spread(ci, feats, parts, 0, top, low)
    unit_hot(ci, hot_out)
    hot = hot_out[...]
    both = dot_nt(hot, top[...]) + dot_nt(hot, low[...])
    glob = [gp[a] for a in range(GPAR)]
    sums = totals_row([weight * glob[a] * glob[b] for a, b in pairs(GPAR)], G_COL)
    left_out[...] = both[:, :LANES]
    right_out[...] = both[:, LANES:] + sums


def sweep_kernel(
    own, left, right, kn, first_in, ph, ap, w, cp, ci, gp, hot, zl, zr, second_out, step_out, z_out, ext, parts, top, low
):
    lane = lax.broadcasted_iota(jnp.int32, (32, LANES), 1)
    summed = own[...]
    summed = summed + jnp.where(lane < 12, pltpu.roll(left[...], 32, 1), 0.0)
    summed = summed + jnp.where((lane >= 105) & (lane < 117), pltpu.roll(right[...], 96, 1), 0.0)
    ext[...] = summed
    row = [ext[r : r + 1, :] for r in range(27)]
    base = jnp.broadcast_to(kn[0:1, 0:1] & ~(KPT - 1), (1, LANES))
    node = base + lax.broadcasted_iota(jnp.int32, (1, LANES), 1) - HALO
    exists = (node >= 0) & (node < NODES)
    rhs = row[0:3]
    band = [row[3 + 6 * d : 9 + 6 * d] for d in range(4)]
    low3, inv3 = factor(band[0], 3)

    def precondition(vector):
        return [OMEGA * v for v in backward(low3, inv3, forward(low3, inv3, vector))]

    def times(values, x, a):
        out = entry(values, 3, a, 0) * x[0]
        out = out + entry(values, 3, a, 1) * x[1]
        return out + entry(values, 3, a, 2) * x[2]

    def kept(values):
        return [jnp.where(exists, v, 0.0) for v in values]

    x = kept(precondition(rhs))
    for _ in range(1, ATT_SWEEPS):
        rest = [rhs[a] - x[a] - times(band[0], x, a) for a in range(3)]
        for d in range(1, 4):
            ahead = [pltpu.roll(v, LANES - d, 1) for v in x]
            for a in range(3):
                rest[a] = rest[a] - times(band[d], ahead, a)
                rest[a] = rest[a] - pltpu.roll(times(band[d], x, a), d, 1)
        step = precondition(rest)
        x = kept([x[a] + step[a] for a in range(3)])
    for c in range(3):
        value = low3[c][c] * x[c]
        for k in range(c + 1, 3):
            value = value + low3[k][c] * x[k]
        step_out[c : c + 1, :] = pltpu.roll(value, LANES - HALO, 1)[:, :ND]
    tile = lax.broadcasted_iota(jnp.int32, (TILES, LANES), 0)
    local = (kn[...] & (KPT - 1)) + KPT * tile + HALO
    basis = spline(ph[...])
    att = [ap[a] for a in range(3)]
    spread_x = [jnp.broadcast_to(v, (TILES, LANES)) for v in x]
    second = first_in[...]
    for i in range(4):
        dot = att[0] * jnp.take_along_axis(spread_x[0], local + i, axis=1)
        for a in range(1, 3):
            dot = dot + att[a] * jnp.take_along_axis(spread_x[a], local + i, axis=1)
        second = second - basis[i] * dot
    second_out[...] = second
    push = w[...] * second
    feats = [push * cp[a] for a in range(CPAR)]
    top[...] = jnp.zeros_like(top)
    low[...] = jnp.zeros_like(low)
    spread(ci, feats, parts, E_COL, top, low)
    both = dot_nt(hot[...], top[...]) + dot_nt(hot[...], low[...])
    sums = totals_row([push * gp[a] for a in range(GPAR)], H_COL)
    z_out[pl.ds(0, LO, stride=2), :] = zl[...]
    z_out[pl.ds(1, LO, stride=2), :] = zr[...] + both + sums


def at_lane(row, start):
    return pltpu.roll(row, (LANES - start) % LANES, 1) if start else row


def solve_kernel(z, row_out, glob_out, fold):
    parts = [z[8 * k : 8 * k + 8, :] for k in range(z.shape[0] // 8)]
    while len(parts) > 1:
        parts = [a + b for a, b in zip(parts[::2], parts[1::2])]
    fold[...] = parts[0]
    left = fold[0:1, :] + fold[2:3, :] + fold[4:5, :] + fold[6:7, :]
    right = fold[1:2, :] + fold[3:4, :] + fold[5:6, :] + fold[7:8, :]
    columns = [at_lane(left if f < 16 else right, f * HI % LANES) for f in range(N_C + CPAR)]
    low6, inv6 = factor(columns[:N_C], CPAR)
    white = forward(low6, inv6, columns[N_C:])
    solved = backward(low6, inv6, white)
    lane = lax.broadcasted_iota(jnp.int32, (1, LANES), 1)
    row = jnp.zeros((1, LANES), F32)
    for j, value in enumerate(white + solved):
        moved = pltpu.roll(value, j * HI, 1) if j else value
        row = jnp.where((lane >= j * HI) & (lane < (j + 1) * HI), moved, row)
    row_out[...] = jnp.broadcast_to(row, row_out.shape)
    glob = [at_lane(right, G_COL + k) for k in range(N_G + GPAR)]
    low4, inv4 = factor(glob[:N_G], GPAR)
    white4 = forward(low4, inv4, glob[N_G:])
    solved4 = backward(low4, inv4, white4)
    for k, value in enumerate(white4 + solved4):
        glob_out[k : k + 1, :] = value


def final_kernel(table, second, cp, ci, gp, glob, res_out, calib_out, rows):
    rows[:, 0:LANES] = jnp.transpose(table[0:LANES, :])
    rows[:, LANES:] = jnp.transpose(table[LANES:, :])
    for j in range(CPAR):
        for h in range(HI):
            calib_out[j : j + 1, h * LO : (h + 1) * LO] = rows[j * HI + h : j * HI + h + 1, :]
    unit = ci[...]
    row_id = unit >> 7
    lane_id = unit & (LANES - 1)
    picked = [jnp.zeros((TILES, LANES), F32) for _ in range(CPAR)]
    for h in range(2 * HI):
        mine = row_id == h
        half = (h & 1) * LANES
        for c in range(CPAR):
            at = (CPAR + c) * HI + (h >> 1)
            row = jnp.broadcast_to(rows[at : at + 1, half : half + LANES], (TILES, LANES))
            picked[c] = jnp.where(mine, jnp.take_along_axis(row, lane_id, axis=1), picked[c])
    total = cp[0] * picked[0]
    for c in range(1, CPAR):
        total = total + cp[c] * picked[c]
    out = second[...] - total
    shift = gp[0] * glob[GPAR : GPAR + 1, 0:1]
    for a in range(1, GPAR):
        shift = shift + gp[a] * glob[GPAR + a : GPAR + a + 1, 0:1]
    res_out[...] = out - shift


NODES = 3072


def shifted(x, by):
    count = lax.axis_size("tm")
    return lax.ppermute(x, "tm", [(i, i + by) for i in range(count) if 0 <= i + by < count])


def call(kernel, outs, scratch, *args, flops=0):
    out_shape = [jax.ShapeDtypeStruct(s, d) for s, d in outs]
    return pl.pallas_call(
        kernel,
        out_shape=out_shape,
        scratch_shapes=[pltpu.VMEM(s, d) for s, d in scratch],
        cost_estimate=pl.CostEstimate(flops=flops, transcendentals=0, bytes_accessed=1 << 20),
    )(*args)


def per_device(res, w, sp, si, sd, ap, ph, kn, cp, ci, gp):
    tiles = (TILES, LANES)
    rows = TILES * LANES
    res, w, si, ph, kn, ci = (x.reshape(tiles) for x in (res, w, si, ph, kn, ci))
    sp, ap, cp, gp = (x.reshape(x.shape[0], *tiles) for x in (sp, ap, cp, gp))
    sd = sd.reshape(SPAR, -1, LANES)
    feat_rows = sum(BASES)
    padded = -(-feat_rows // 16) * 16
    first, att = call(
        attitude_kernel,
        [(tiles, F32), ((32, LANES), F32)],
        [((feat_rows * TILES, LANES), F32), ((2 * padded, rows), BF16), ((LANES, rows), BF16), ((padded, LANES), F32)],
        res, w, sp, si, sd, ap, ph, kn, flops=1 << 24,
    )
    groups = lax.axis_size("grp")
    copies = jnp.broadcast_to(att, (groups, *att.shape))
    gathered = lax.all_to_all(copies, "grp", split_axis=0, concat_axis=0, tiled=True)
    zl, zr, hot = call(
        matrix_kernel,
        [((LO, LANES), F32), ((LO, LANES), F32), ((LO, rows), BF16)],
        [((2, N_C * TILES, LANES), F32), ((2 * LANES, rows), BF16), ((2 * LANES, rows), BF16)],
        w, cp, ci, gp, flops=1 << 25,
    )
    own = gathered.sum(axis=0)
    left = shifted(own, 1)
    right = shifted(own, -1)
    second, step, z = call(
        sweep_kernel,
        [(tiles, F32), ((3, ND), F32), ((2 * LO, LANES), F32)],
        [((32, LANES), F32), ((2, CPAR * TILES, LANES), F32), ((LANES, rows), BF16), ((LANES, rows), BF16)],
        own, left, right, kn, first, ph, ap, w, cp, ci, gp, hot, zl, zr, flops=1 << 24,
    )
    both = ("tm", "grp")
    z = lax.all_to_all(z.reshape(LO, 2, LANES), both, split_axis=0, concat_axis=0, tiled=True)
    copies, glob = call(
        solve_kernel,
        [((LO, LANES), F32), ((2 * GPAR, LANES), F32)],
        [((8, LANES), F32)],
        z.reshape(2 * LO, LANES),
    )
    table = lax.all_to_all(copies.reshape(LO, 1, LANES), both, split_axis=0, concat_axis=0, tiled=True)
    out, calib = call(
        final_kernel,
        [(tiles, F32), ((CPAR, UNITS), F32)],
        [((LANES, LO), F32)],
        table.reshape(LO, LANES), second, cp, ci, gp, glob,
    )
    return out.reshape(1, 1, rows), step, calib, glob[:GPAR, 0]


def solution(mesh):
    return jax.shard_map(
        per_device,
        mesh=mesh,
        in_specs=(
            P("tm", "grp", None),
            P("tm", "grp", None),
            P(None, "tm", "grp", None),
            P("tm", "grp", None),
            P(None, "tm", None),
            P(None, "tm", "grp", None),
            P("tm", "grp", None),
            P("tm", "grp", None),
            P(None, "tm", "grp", None),
            P("tm", "grp", None),
            P(None, "tm", "grp", None),
        ),
        out_specs=(P("tm", "grp", None), P(None, "tm"), P(), P()),
        check_vma=False,
    )
```

```python
import jax
import jax.numpy as jnp
from jax import lax
from jax.experimental import pallas as pl
from jax.experimental.pallas import tpu as pltpu
from jax.sharding import PartitionSpec as P

LANES = 128
TILES = 24
KPT = 4
UNITS = 2048
CPAR = 6
GPAR = 4
SPAR = 5
ATT_SWEEPS = 4
ND = 96
HALO = 9
OMEGA = 0.6
RIDGE = 1.0
HI = 8
LO = 256
CHUNK = 8
BAND = 24
F32 = jnp.float32
BF16 = jnp.bfloat16


def pairs(extent):
    return [(a, b) for a in range(extent) for b in range(a, extent)]


PAIR_AT = {extent: {p: i for i, p in enumerate(pairs(extent))} for extent in (3, 4, 6)}


def entry(values, extent, a, b):
    return values[PAIR_AT[extent][(min(a, b), max(a, b))]]


def factor(values, extent):
    low = [[None] * extent for _ in range(extent)]
    inv = [None] * extent
    for c in range(extent):
        pivot = entry(values, extent, c, c) + RIDGE
        for k in range(c):
            pivot = pivot - low[c][k] * low[c][k]
        low[c][c] = jnp.sqrt(pivot)
        inv[c] = 1.0 / low[c][c]
        for r in range(c + 1, extent):
            value = entry(values, extent, r, c)
            for k in range(c):
                value = value - low[r][k] * low[c][k]
            low[r][c] = value * inv[c]
    return low, inv


def forward(low, inv, vector):
    out = []
    for r in range(len(vector)):
        value = vector[r]
        for k in range(r):
            value = value - low[r][k] * out[k]
        out.append(value * inv[r])
    return out


def backward(low, inv, vector):
    extent = len(vector)
    out = [None] * extent
    for r in reversed(range(extent)):
        value = vector[r]
        for k in range(r + 1, extent):
            value = value - low[k][r] * out[k]
        out[r] = value * inv[r]
    return out


def spline(u):
    v = 1.0 - u
    s = u * u
    c = s * u
    sixth = 1.0 / 6.0
    return [
        v * v * v * sixth,
        (3.0 * c - 6.0 * s + 4.0) * sixth,
        (-3.0 * c + 3.0 * s + 3.0 * u + 1.0) * sixth,
        c * sixth,
    ]


def halves(x):
    top = x.astype(BF16).astype(F32)
    return top, x - top


def dot_nt(a, b):
    return lax.dot_general(a, b, (((1,), (1,)), ((), ())), preferred_element_type=F32)


def attitude_kernel(*refs):
    far, refs = refs[:11], refs[11:]
    (first_out, att_out), near, refs = refs[:2], refs[2:9], refs[9:]
    near, refs = (*near, *refs[:4]), refs[4:]
    feat, lhs, rhs_feat, rhs, hot, acc, shut, sems = refs
    loads = [pltpu.make_async_copy(a, b, sems.at[i]) for i, (a, b) in enumerate(zip(far, near))]
    for i in (10, 9, 0, 1, 2, 3, 8, 7, 4, 5, 6):
        loads[i].start()
    w, ap, ph, kn, cp, ci, gp, res, sp, si, sd = near
    for i in (10, 9, 0, 1, 2, 3, 8, 7):
        loads[i].wait()
    basis = spline(ph[...])
    weight = w[...]
    att = [ap[a] for a in range(3)]
    outer = [weight * att[a] * att[b] for a, b in pairs(3)]
    at = 0
    for i in range(4):
        for d in range(4 - i):
            both = basis[i] * basis[i + d]
            for value in outer:
                feat[pl.ds(at * TILES, TILES), :] = both * value
                at += 1
    count = at
    node = lax.broadcasted_iota(jnp.int32, (LANES, LANES), 0)
    index = si[...]
    row_id = index >> 7
    lane_id = index & (LANES - 1)
    picked = [jnp.zeros((TILES, LANES), F32) for _ in range(SPAR)]
    half = lhs.shape[0] // 2
    band = None
    steps = TILES // CHUNK
    for s in range(steps):
        for t in range(s * CHUNK, (s + 1) * CHUNK):
            cols = slice(t * LANES, (t + 1) * LANES)
            top, low = halves(feat[pl.ds(t, count, stride=TILES), :])
            lhs[0:count, cols] = top.astype(BF16)
            lhs[half : half + count, cols] = low.astype(BF16)
            slot = (kn[t : t + 1, :] & (KPT - 1)) + (KPT * t + HALO)
            hot[:, cols] = jnp.where(node == slot, 1.0, 0.0).astype(BF16)
        cols = slice(s * CHUNK * LANES, (s + 1) * CHUNK * LANES)
        part = dot_nt(lhs[:, cols], hot[:, cols])
        band = part if band is None else band + part
        for h in range(s * sd.shape[1] // steps, (s + 1) * sd.shape[1] // steps):
            mine = row_id == h
            for c in range(SPAR):
                row = jnp.broadcast_to(sd[c, h : h + 1, :], (TILES, LANES))
                picked[c] = jnp.where(mine, jnp.take_along_axis(row, lane_id, axis=1), picked[c])
    acc[...] = band[:half] + band[half:]
    total = sp[0] * picked[0]
    for c in range(1, SPAR):
        total = total + sp[c] * picked[c]
    first = res[...] - total
    first_out[...] = first
    at = 0
    for i in range(4):
        for a in range(3):
            rhs_feat[pl.ds(at * TILES, TILES), :] = basis[i] * (weight * att[a] * first)
            at += 1
    for t in range(TILES):
        cols = slice(t * LANES, (t + 1) * LANES)
        top, low = halves(rhs_feat[pl.ds(t, at, stride=TILES), :])
        rhs[0:at, cols] = top.astype(BF16)
        rhs[16 : 16 + at, cols] = low.astype(BF16)
    both = dot_nt(rhs[...], hot[...])
    both = both[:16] + both[16:]
    shut[...] = jnp.zeros_like(shut)
    at = 0
    side = both[0:3]
    for i in range(4):
        rows = 6 * (4 - i)
        value = acc[at : at + rows, :]
        if i:
            value = pltpu.roll(value, i, 1)
            side = side + pltpu.roll(both[3 * i : 3 * i + 3, :], i, 1)
        shut[0:rows, :] = shut[0:rows, :] + value
        at += rows
    shut[BAND : BAND + 3, :] = side
    att_out[...] = jnp.broadcast_to(shut[...][None], att_out.shape)
    for i in (4, 5, 6):
        loads[i].wait()


def unit_hot(unit, hot):
    lo_id = lax.broadcasted_iota(jnp.int32, (LO, LANES), 0)
    for t in range(TILES):
        cols = slice(t * LANES, (t + 1) * LANES)
        lo = unit[t : t + 1, :] & (LO - 1)
        hot[:, cols] = jnp.where(lo_id == lo, 1.0, 0.0).astype(BF16)


def spread(unit, feats, parts, top_to, low_to):
    for f, value in enumerate(feats):
        top, low = halves(value)
        parts[0, pl.ds(f * TILES, TILES), :] = top
        parts[1, pl.ds(f * TILES, TILES), :] = low
    hi_id = lax.broadcasted_iota(jnp.int32, (HI, LANES), 0)
    zero = jnp.zeros((HI, LANES), F32)
    for t in range(TILES):
        cols = slice(t * LANES, (t + 1) * LANES)
        mine = hi_id == (unit[t : t + 1, :] >> 8)
        for part, (to, base) in ((0, top_to), (1, low_to)):
            for f in range(0, len(feats), 2):
                rows = []
                for g in (f, f + 1):
                    if g < len(feats):
                        row = parts[part, g * TILES + t : g * TILES + t + 1, :]
                        rows.append(jnp.where(mine, jnp.broadcast_to(row, (HI, LANES)), 0.0))
                    else:
                        rows.append(zero)
                at = (base + f * HI) % to.shape[0]
                to[at : at + 2 * HI, cols] = jnp.concatenate(rows, axis=0).astype(BF16)


def totals_row(values, first_lane):
    lane = lax.broadcasted_iota(jnp.int32, (1, LANES), 1)
    row = jnp.zeros((1, LANES), F32)
    for k, value in enumerate(values):
        folded = value[0:8] + value[8:16] + value[16:24]
        total = jnp.sum(jnp.sum(folded, axis=1, keepdims=True), axis=0, keepdims=True)
        row = jnp.where(lane == first_lane + k, total, row)
    return row


N_C = CPAR * (CPAR + 1) // 2
N_G = GPAR * (GPAR + 1) // 2
E_COL = (N_C + 1) // 2 * 2 * HI - LANES
G_COL = E_COL + CPAR * HI
H_COL = G_COL + N_G


def matrix_kernel(w, cp, ci, gp, left_out, right_out, hot_out, parts, top, low):
    weight = w[...]
    calib = [cp[a] for a in range(CPAR)]
    weighted = [weight * c for c in calib]
    feats = [weighted[a] * calib[b] for a, b in pairs(CPAR)]
    used = (N_C + 1) // 2 * 2 * HI
    top[used:, :] = jnp.zeros((2 * LANES - used, top.shape[1]), BF16)
    low[used:, :] = jnp.zeros((2 * LANES - used, top.shape[1]), BF16)
    spread(ci, feats, parts, (top, 0), (low, 0))
    unit_hot(ci, hot_out)
    hot = hot_out[...]
    both = dot_nt(hot, top[...]) + dot_nt(hot, low[...])
    glob = [gp[a] for a in range(GPAR)]
    sums = totals_row([weight * glob[a] * glob[b] for a, b in pairs(GPAR)], G_COL)
    left_out[...] = both[:, :LANES]
    right_out[...] = both[:, LANES:] + sums


def sweep_kernel(
    own, inside, outside, kn, first_in, ph, ap, w, cp, ci, gp, hot, zl, zr, second_out, step_out, z_out, ext, parts, mid
):
    lane = lax.broadcasted_iota(jnp.int32, own.shape, 1)
    base = jnp.broadcast_to(kn[0:1, 0:1] & ~(KPT - 1), (1, LANES))
    odd = ((base >> 5) & 1) == 1
    left = jnp.where(odd, inside[...], outside[...])
    right = jnp.where(odd, outside[...], inside[...])
    at_left = lane < HALO + 3
    at_right = (lane >= HALO + ND) & (lane < HALO + ND + 12)
    ext[...] = (
        own[...]
        + jnp.where(at_left, pltpu.roll(left, LANES - ND, 1), 0.0)
        + jnp.where(at_right, pltpu.roll(right, ND, 1), 0.0)
    )
    row = [ext[r : r + 1, :] for r in range(BAND + 3)]
    node = base + lax.broadcasted_iota(jnp.int32, (1, LANES), 1) - HALO
    exists = (node >= 0) & (node < NODES)
    rhs = row[BAND:]
    band = [row[6 * d : 6 * d + 6] for d in range(4)]
    low3, inv3 = factor(band[0], 3)

    def precondition(vector):
        return [OMEGA * v for v in backward(low3, inv3, forward(low3, inv3, vector))]

    def times(values, x, a):
        out = entry(values, 3, a, 0) * x[0]
        out = out + entry(values, 3, a, 1) * x[1]
        return out + entry(values, 3, a, 2) * x[2]

    def kept(values):
        return [jnp.where(exists, v, 0.0) for v in values]

    x = kept(precondition(rhs))
    for _ in range(1, ATT_SWEEPS):
        rest = [rhs[a] - x[a] - times(band[0], x, a) for a in range(3)]
        for d in range(1, 4):
            ahead = [pltpu.roll(v, LANES - d, 1) for v in x]
            for a in range(3):
                rest[a] = rest[a] - times(band[d], ahead, a)
                rest[a] = rest[a] - pltpu.roll(times(band[d], x, a), d, 1)
        step = precondition(rest)
        x = kept([x[a] + step[a] for a in range(3)])
    for c in range(3):
        value = low3[c][c] * x[c]
        for k in range(c + 1, 3):
            value = value + low3[k][c] * x[k]
        step_out[c : c + 1, :] = pltpu.roll(value, LANES - HALO, 1)[:, :ND]
    tile = lax.broadcasted_iota(jnp.int32, (TILES, LANES), 0)
    local = (kn[...] & (KPT - 1)) + KPT * tile + HALO
    basis = spline(ph[...])
    att = [ap[a] for a in range(3)]
    spread_x = [jnp.broadcast_to(v, (TILES, LANES)) for v in x]
    second = first_in[...]
    for i in range(4):
        dot = att[0] * jnp.take_along_axis(spread_x[0], local + i, axis=1)
        for a in range(1, 3):
            dot = dot + att[a] * jnp.take_along_axis(spread_x[a], local + i, axis=1)
        second = second - basis[i] * dot
    second_out[...] = second
    push = w[...] * second
    feats = [push * cp[a] for a in range(CPAR)]
    half = LANES // 2
    for row in (E_COL - half // 4, E_COL + half - half // 4):
        mid[row : row + half // 4, :] = jnp.zeros((half // 4, mid.shape[1]), BF16)
    spread(ci, feats, parts, (mid, E_COL), (mid, E_COL + half))
    both = dot_nt(hot[...], mid[...])
    lane = lax.broadcasted_iota(jnp.int32, both.shape, 1)
    both = jnp.where((lane >= E_COL) & (lane < G_COL), both + pltpu.roll(both, half, 1), 0.0)
    sums = totals_row([push * gp[a] for a in range(GPAR)], H_COL)
    z_out[pl.ds(0, LO, stride=2), :] = zl[...]
    z_out[pl.ds(1, LO, stride=2), :] = zr[...] + both + sums


def at_lane(row, start):
    return pltpu.roll(row, (LANES - start) % LANES, 1) if start else row


def solve_kernel(z, row_out, glob_out, step_out, fold):
    parts = [z[8 * k : 8 * k + 8, :] for k in range(z.shape[0] // 8)]
    while len(parts) > 1:
        parts = [a + b for a, b in zip(parts[::2], parts[1::2])]
    fold[...] = parts[0]
    left = fold[0:1, :] + fold[2:3, :] + fold[4:5, :] + fold[6:7, :]
    right = fold[1:2, :] + fold[3:4, :] + fold[5:6, :] + fold[7:8, :]
    columns = [at_lane(left if f < 16 else right, f * HI % LANES) for f in range(N_C)]
    columns += [at_lane(right, E_COL + f * HI) for f in range(CPAR)]
    low6, inv6 = factor(columns[:N_C], CPAR)
    white = forward(low6, inv6, columns[N_C:])
    solved = backward(low6, inv6, white)
    lane = lax.broadcasted_iota(jnp.int32, (1, LANES), 1)
    row = jnp.zeros((1, LANES), F32)
    for j, value in enumerate(white + solved):
        moved = pltpu.roll(value, j * HI, 1) if j else value
        row = jnp.where((lane >= j * HI) & (lane < (j + 1) * HI), moved, row)
    row_out[...] = jnp.broadcast_to(row, row_out.shape)
    glob = [at_lane(right, G_COL + k) for k in range(N_G + GPAR)]
    low4, inv4 = factor(glob[:N_G], GPAR)
    white4 = forward(low4, inv4, glob[N_G:])
    solved4 = backward(low4, inv4, white4)
    for k, value in enumerate(solved4):
        glob_out[k : k + 1, :] = value
    row = white4[0]
    for k in range(1, GPAR):
        row = jnp.where(lane == k, pltpu.roll(white4[k], k, 1), row)
    step_out[...] = row[:, :GPAR]


def final_kernel(table, second, cp, ci, gp, glob, res_out, calib_out, rows):
    rows[:, 0:LANES] = jnp.transpose(table[0:LANES, :])
    rows[:, LANES:] = jnp.transpose(table[LANES:, :])
    for j in range(CPAR):
        for h in range(HI):
            calib_out[j : j + 1, h * LO : (h + 1) * LO] = rows[j * HI + h : j * HI + h + 1, :]
    unit = ci[...]
    row_id = unit >> 7
    lane_id = unit & (LANES - 1)
    picked = [jnp.zeros((TILES, LANES), F32) for _ in range(CPAR)]
    for h in range(2 * HI):
        mine = row_id == h
        half = (h & 1) * LANES
        for c in range(CPAR):
            at = (CPAR + c) * HI + (h >> 1)
            row = jnp.broadcast_to(rows[at : at + 1, half : half + LANES], (TILES, LANES))
            picked[c] = jnp.where(mine, jnp.take_along_axis(row, lane_id, axis=1), picked[c])
    total = cp[0] * picked[0]
    for c in range(1, CPAR):
        total = total + cp[c] * picked[c]
    out = second[...] - total
    shift = gp[0] * glob[0:1, 0:1]
    for a in range(1, GPAR):
        shift = shift + gp[a] * glob[a : a + 1, 0:1]
    res_out[...] = out - shift


NODES = 3072


def paired(x, start):
    count = lax.axis_size("tm")
    low = range(start, count - 1, 2)
    return lax.ppermute(x, "tm", [(i, i + 1) for i in low] + [(i + 1, i) for i in low])


def call(kernel, outs, scratch, *args, flops=0, limit=16 << 20, far=False):
    out_shape = [jax.ShapeDtypeStruct(s, d) for s, d in outs]
    vmem = pl.BlockSpec(memory_space=pltpu.VMEM)
    given = pl.BlockSpec(memory_space=pltpu.HBM) if far else vmem
    return pl.pallas_call(
        kernel,
        out_shape=out_shape,
        in_specs=[given] * len(args),
        out_specs=[vmem] * len(outs),
        scratch_shapes=scratch,
        compiler_params=pltpu.CompilerParams(vmem_limit_bytes=limit),
        cost_estimate=pl.CostEstimate(flops=flops, transcendentals=0, bytes_accessed=1 << 20),
    )(*(pltpu.with_memory_space_constraint(a, pltpu.HBM) if far else a for a in args))


def per_device(res, w, sp, si, sd, ap, ph, kn, cp, ci, gp):
    tiles = (TILES, LANES)
    rows = TILES * LANES
    vmem = pltpu.VMEM
    res, w, si, ph, kn, ci = (x.reshape(tiles) for x in (res, w, si, ph, kn, ci))
    sp, ap, cp, gp = (x.reshape(x.shape[0], *tiles) for x in (sp, ap, cp, gp))
    sd = sd.reshape(SPAR, -1, LANES)
    groups = lax.axis_size("grp")
    kept = [(x.shape, x.dtype) for x in (w, ap, ph, kn, cp, ci, gp)]
    first, copies, w, ap, ph, kn, cp, ci, gp = call(
        attitude_kernel,
        [(tiles, F32), ((groups, 32, LANES), F32)] + kept,
        [vmem(x.shape, x.dtype) for x in (res, sp, si, sd)]
        + [
            vmem((60 * TILES, LANES), F32),
            vmem((LANES, rows), BF16),
            vmem((12 * TILES, LANES), F32),
            vmem((32, rows), BF16),
            vmem((LANES, rows), BF16),
            vmem((LANES // 2, LANES), F32),
            vmem((32, LANES), F32),
            pltpu.SemaphoreType.DMA((11,)),
        ],
        w, ap, ph, kn, cp, ci, gp, res, sp, si, sd, flops=1 << 24, far=True,
    )
    gathered = lax.all_to_all(copies, "grp", split_axis=0, concat_axis=0, tiled=True)
    zl, zr, hot = call(
        matrix_kernel,
        [((LO, LANES), F32), ((LO, LANES), F32), ((LO, rows), BF16)],
        [vmem((2, N_C * TILES, LANES), F32), vmem((2 * LANES, rows), BF16), vmem((2 * LANES, rows), BF16)],
        w, cp, ci, gp, flops=1 << 27,
    )
    own = gathered.sum(axis=0)
    outside = paired(own, 1)
    inside = paired(own, 0)
    second, step, z = call(
        sweep_kernel,
        [(tiles, F32), ((3, ND), F32), ((2 * LO, LANES), F32)],
        [vmem((32, LANES), F32), vmem((2, CPAR * TILES, LANES), F32), vmem((LANES, rows), BF16)],
        own, inside, outside, kn, first, ph, ap, w, cp, ci, gp, hot, zl, zr, flops=1 << 24,
    )
    both = ("tm", "grp")
    z = lax.all_to_all(z.reshape(LO, 2, LANES), both, split_axis=0, concat_axis=0, tiled=True)
    copies, glob, glob_step = call(
        solve_kernel,
        [((LO, LANES), F32), ((2 * GPAR, LANES), F32), ((1, GPAR), F32)],
        [vmem((8, LANES), F32)],
        z.reshape(2 * LO, LANES),
    )
    table = lax.all_to_all(copies.reshape(LO, 1, LANES), both, split_axis=0, concat_axis=0, tiled=True)
    out, calib = call(
        final_kernel,
        [(tiles, F32), ((CPAR, UNITS), F32)],
        [vmem((LANES, LO), F32)],
        table.reshape(LO, LANES), second, cp, ci, gp, glob,
    )
    return out.reshape(1, 1, rows), step, calib, glob_step.reshape(GPAR)


def solution(mesh):
    return jax.shard_map(
        per_device,
        mesh=mesh,
        in_specs=(
            P("tm", "grp", None),
            P("tm", "grp", None),
            P(None, "tm", "grp", None),
            P("tm", "grp", None),
            P(None, "tm", None),
            P(None, "tm", "grp", None),
            P("tm", "grp", None),
            P("tm", "grp", None),
            P(None, "tm", "grp", None),
            P("tm", "grp", None),
            P(None, "tm", "grp", None),
        ),
        out_specs=(P("tm", "grp", None), P(None, "tm"), P(), P()),
        check_vma=False,
    )
```

```python
import jax
import jax.numpy as jnp
from jax import lax
from jax.experimental import pallas as pl
from jax.experimental.pallas import tpu as pltpu
from jax.sharding import Mesh
from jax.sharding import PartitionSpec as P

LANES = 128
TILES = 24
KPT = 4
UNITS = 2048
CPAR = 6
GPAR = 4
SPAR = 5
ATT_SWEEPS = 4
ND = 96
HALO = 9
OMEGA = 0.6
RIDGE = 1.0
HI = 8
LO = 256
CHUNK = 8
BAND = 24
F32 = jnp.float32
BF16 = jnp.bfloat16


def pairs(extent):
    return [(a, b) for a in range(extent) for b in range(a, extent)]


PAIR_AT = {extent: {p: i for i, p in enumerate(pairs(extent))} for extent in (3, 4, 6)}


def entry(values, extent, a, b):
    return values[PAIR_AT[extent][(min(a, b), max(a, b))]]


def factor(values, extent):
    low = [[None] * extent for _ in range(extent)]
    inv = [None] * extent
    for c in range(extent):
        pivot = entry(values, extent, c, c) + RIDGE
        for k in range(c):
            pivot = pivot - low[c][k] * low[c][k]
        low[c][c] = jnp.sqrt(pivot)
        inv[c] = 1.0 / low[c][c]
        for r in range(c + 1, extent):
            value = entry(values, extent, r, c)
            for k in range(c):
                value = value - low[r][k] * low[c][k]
            low[r][c] = value * inv[c]
    return low, inv


def forward(low, inv, vector):
    out = []
    for r in range(len(vector)):
        value = vector[r]
        for k in range(r):
            value = value - low[r][k] * out[k]
        out.append(value * inv[r])
    return out


def backward(low, inv, vector):
    extent = len(vector)
    out = [None] * extent
    for r in reversed(range(extent)):
        value = vector[r]
        for k in range(r + 1, extent):
            value = value - low[k][r] * out[k]
        out[r] = value * inv[r]
    return out


def spline(u):
    v = 1.0 - u
    s = u * u
    c = s * u
    sixth = 1.0 / 6.0
    return [
        v * v * v * sixth,
        (3.0 * c - 6.0 * s + 4.0) * sixth,
        (-3.0 * c + 3.0 * s + 3.0 * u + 1.0) * sixth,
        c * sixth,
    ]


def halves(x):
    top = x.astype(BF16).astype(F32)
    return top, x - top


def dot_nt(a, b):
    return lax.dot_general(a, b, (((1,), (1,)), ((), ())), preferred_element_type=F32)


def attitude_kernel(*refs):
    far, refs = refs[:11], refs[11:]
    (first_out, att_out), near, refs = refs[:2], refs[2:9], refs[9:]
    near, refs = (*near, *refs[:4]), refs[4:]
    feat, lhs, rhs_feat, rhs, hot, acc, shut, sems = refs
    loads = [pltpu.make_async_copy(a, b, sems.at[i]) for i, (a, b) in enumerate(zip(far, near))]
    for i in (10, 9, 0, 1, 2, 3, 8, 7, 4, 5, 6):
        loads[i].start()
    w, ap, ph, kn, cp, ci, gp, res, sp, si, sd = near
    for i in (10, 9, 0, 1, 2, 3, 8, 7):
        loads[i].wait()
    basis = spline(ph[...])
    weight = w[...]
    att = [ap[a] for a in range(3)]
    outer = [weight * att[a] * att[b] for a, b in pairs(3)]
    at = 0
    for i in range(4):
        for d in range(4 - i):
            both = basis[i] * basis[i + d]
            for value in outer:
                feat[pl.ds(at * TILES, TILES), :] = both * value
                at += 1
    count = at
    node = lax.broadcasted_iota(jnp.int32, (LANES, LANES), 0)
    index = si[...]
    row_id = index >> 7
    lane_id = index & (LANES - 1)
    picked = [jnp.zeros((TILES, LANES), F32) for _ in range(SPAR)]
    half = lhs.shape[0] // 2
    band = None
    steps = TILES // CHUNK
    for s in range(steps):
        for t in range(s * CHUNK, (s + 1) * CHUNK):
            cols = slice(t * LANES, (t + 1) * LANES)
            top, low = halves(feat[pl.ds(t, count, stride=TILES), :])
            lhs[0:count, cols] = top.astype(BF16)
            lhs[half : half + count, cols] = low.astype(BF16)
            slot = (kn[t : t + 1, :] & (KPT - 1)) + (KPT * t + HALO)
            hot[:, cols] = jnp.where(node == slot, 1.0, 0.0).astype(BF16)
        cols = slice(s * CHUNK * LANES, (s + 1) * CHUNK * LANES)
        part = dot_nt(lhs[:, cols], hot[:, cols])
        band = part if band is None else band + part
        for h in range(s * sd.shape[1] // steps, (s + 1) * sd.shape[1] // steps):
            mine = row_id == h
            for c in range(SPAR):
                row = jnp.broadcast_to(sd[c, h : h + 1, :], (TILES, LANES))
                picked[c] = jnp.where(mine, jnp.take_along_axis(row, lane_id, axis=1), picked[c])
    acc[...] = band[:half] + band[half:]
    total = sp[0] * picked[0]
    for c in range(1, SPAR):
        total = total + sp[c] * picked[c]
    first = res[...] - total
    first_out[...] = first
    at = 0
    for i in range(4):
        for a in range(3):
            rhs_feat[pl.ds(at * TILES, TILES), :] = basis[i] * (weight * att[a] * first)
            at += 1
    for t in range(TILES):
        cols = slice(t * LANES, (t + 1) * LANES)
        top, low = halves(rhs_feat[pl.ds(t, at, stride=TILES), :])
        rhs[0:at, cols] = top.astype(BF16)
        rhs[16 : 16 + at, cols] = low.astype(BF16)
    both = dot_nt(rhs[...], hot[...])
    both = both[:16] + both[16:]
    shut[...] = jnp.zeros_like(shut)
    at = 0
    side = both[0:3]
    for i in range(4):
        rows = 6 * (4 - i)
        value = acc[at : at + rows, :]
        if i:
            value = pltpu.roll(value, i, 1)
            side = side + pltpu.roll(both[3 * i : 3 * i + 3, :], i, 1)
        shut[0:rows, :] = shut[0:rows, :] + value
        at += rows
    shut[BAND : BAND + 3, :] = side
    att_out[...] = jnp.broadcast_to(shut[...][None], att_out.shape)
    for i in (4, 5, 6):
        loads[i].wait()


def unit_hot(unit, flip, hot):
    lo_id = lax.broadcasted_iota(jnp.int32, (LO, LANES), 0)
    for t in range(TILES):
        cols = slice(t * LANES, (t + 1) * LANES)
        lo = (unit[t : t + 1, :] & (LO - 1)) ^ flip
        hot[:, cols] = jnp.where(lo_id == lo, 1.0, 0.0).astype(BF16)


def spread(unit, feats, parts, top_to, low_to):
    for f, value in enumerate(feats):
        top, low = halves(value)
        parts[0, pl.ds(f * TILES, TILES), :] = top
        parts[1, pl.ds(f * TILES, TILES), :] = low
    hi_id = lax.broadcasted_iota(jnp.int32, (HI, LANES), 0)
    zero = jnp.zeros((HI, LANES), F32)
    for t in range(TILES):
        cols = slice(t * LANES, (t + 1) * LANES)
        mine = hi_id == (unit[t : t + 1, :] >> 8)
        for part, (to, base) in ((0, top_to), (1, low_to)):
            for f in range(0, len(feats), 2):
                rows = []
                for g in (f, f + 1):
                    if g < len(feats):
                        row = parts[part, g * TILES + t : g * TILES + t + 1, :]
                        rows.append(jnp.where(mine, jnp.broadcast_to(row, (HI, LANES)), 0.0))
                    else:
                        rows.append(zero)
                at = (base + f * HI) % to.shape[0]
                to[at : at + 2 * HI, cols] = jnp.concatenate(rows, axis=0).astype(BF16)


def totals_row(values, first_lane):
    lane = lax.broadcasted_iota(jnp.int32, (1, LANES), 1)
    row = jnp.zeros((1, LANES), F32)
    for k, value in enumerate(values):
        folded = value[0:8] + value[8:16] + value[16:24]
        total = jnp.sum(jnp.sum(folded, axis=1, keepdims=True), axis=0, keepdims=True)
        row = jnp.where(lane == first_lane + k, total, row)
    return row


N_C = CPAR * (CPAR + 1) // 2
N_G = GPAR * (GPAR + 1) // 2
E_COL = (N_C + 1) // 2 * 2 * HI - LANES
G_COL = E_COL + CPAR * HI
H_COL = G_COL + N_G


def matrix_kernel(w, cp, ci, gp, kn, left_out, right_out, hot_out, parts, top, low):
    weight = w[...]
    calib = [cp[a] for a in range(CPAR)]
    weighted = [weight * c for c in calib]
    feats = [weighted[a] * calib[b] for a, b in pairs(CPAR)]
    used = (N_C + 1) // 2 * 2 * HI
    top[used:, :] = jnp.zeros((2 * LANES - used, top.shape[1]), BF16)
    low[used:, :] = jnp.zeros((2 * LANES - used, top.shape[1]), BF16)
    spread(ci, feats, parts, (top, 0), (low, 0))
    flip = ((kn[0:1, 0:1] >> 5) & 1) << 7
    unit_hot(ci, jnp.broadcast_to(flip, (1, LANES)), hot_out)
    hot = hot_out[...]
    both = dot_nt(hot, top[...]) + dot_nt(hot, low[...])
    glob = [gp[a] for a in range(GPAR)]
    sums = totals_row([weight * glob[a] * glob[b] for a, b in pairs(GPAR)], G_COL)
    left_out[...] = both[:, :LANES]
    right_out[...] = both[:, LANES:] + sums


def sweep_kernel(
    own, inside, outside, kn, first_in, ph, ap, w, cp, ci, gp, hot, zl, zr, second_out, step_out, keep_out, send_out, ext, parts, mid
):
    lane = lax.broadcasted_iota(jnp.int32, own.shape, 1)
    base = jnp.broadcast_to(kn[0:1, 0:1] & ~(KPT - 1), (1, LANES))
    odd = ((base >> 5) & 1) == 1
    left = jnp.where(odd, inside[...], outside[...])
    right = jnp.where(odd, outside[...], inside[...])
    at_left = lane < HALO + 3
    at_right = (lane >= HALO + ND) & (lane < HALO + ND + 12)
    ext[...] = (
        own[...]
        + jnp.where(at_left, pltpu.roll(left, LANES - ND, 1), 0.0)
        + jnp.where(at_right, pltpu.roll(right, ND, 1), 0.0)
    )
    row = [ext[r : r + 1, :] for r in range(BAND + 3)]
    node = base + lax.broadcasted_iota(jnp.int32, (1, LANES), 1) - HALO
    exists = (node >= 0) & (node < NODES)
    rhs = row[BAND:]
    band = [row[6 * d : 6 * d + 6] for d in range(4)]
    low3, inv3 = factor(band[0], 3)

    def precondition(vector):
        return [OMEGA * v for v in backward(low3, inv3, forward(low3, inv3, vector))]

    def times(values, x, a):
        out = entry(values, 3, a, 0) * x[0]
        out = out + entry(values, 3, a, 1) * x[1]
        return out + entry(values, 3, a, 2) * x[2]

    def kept(values):
        return [jnp.where(exists, v, 0.0) for v in values]

    x = kept(precondition(rhs))
    for _ in range(1, ATT_SWEEPS):
        rest = [rhs[a] - x[a] - times(band[0], x, a) for a in range(3)]
        for d in range(1, 4):
            ahead = [pltpu.roll(v, LANES - d, 1) for v in x]
            for a in range(3):
                rest[a] = rest[a] - times(band[d], ahead, a)
                rest[a] = rest[a] - pltpu.roll(times(band[d], x, a), d, 1)
        step = precondition(rest)
        x = kept([x[a] + step[a] for a in range(3)])
    for c in range(3):
        value = low3[c][c] * x[c]
        for k in range(c + 1, 3):
            value = value + low3[k][c] * x[k]
        step_out[c : c + 1, :] = pltpu.roll(value, LANES - HALO, 1)[:, :ND]
    tile = lax.broadcasted_iota(jnp.int32, (TILES, LANES), 0)
    local = (kn[...] & (KPT - 1)) + KPT * tile + HALO
    basis = spline(ph[...])
    att = [ap[a] for a in range(3)]
    spread_x = [jnp.broadcast_to(v, (TILES, LANES)) for v in x]
    second = first_in[...]
    for i in range(4):
        dot = att[0] * jnp.take_along_axis(spread_x[0], local + i, axis=1)
        for a in range(1, 3):
            dot = dot + att[a] * jnp.take_along_axis(spread_x[a], local + i, axis=1)
        second = second - basis[i] * dot
    second_out[...] = second
    push = w[...] * second
    feats = [push * cp[a] for a in range(CPAR)]
    half = LANES // 2
    for row in (E_COL - half // 4, E_COL + half - half // 4):
        mid[row : row + half // 4, :] = jnp.zeros((half // 4, mid.shape[1]), BF16)
    spread(ci, feats, parts, (mid, E_COL), (mid, E_COL + half))
    both = dot_nt(mid[...], hot[...])
    both = jnp.concatenate([jnp.transpose(both[:, :LANES]), jnp.transpose(both[:, LANES:])], axis=0)
    lane = lax.broadcasted_iota(jnp.int32, both.shape, 1)
    both = jnp.where((lane >= E_COL) & (lane < G_COL), both + pltpu.roll(both, half, 1), 0.0)
    sums = totals_row([push * gp[a] for a in range(GPAR)], H_COL)
    right = zr[...] + both + sums
    for to, at in ((keep_out, 0), (send_out, LO // 2)):
        to[pl.ds(0, LO // 2, stride=2), :] = zl[at : at + LO // 2, :]
        to[pl.ds(1, LO // 2, stride=2), :] = right[at : at + LO // 2, :]


def at_lane(row, start):
    return pltpu.roll(row, (LANES - start) % LANES, 1) if start else row


def solve_kernel(z, row_out, glob_out, step_out, fold):
    parts = [z[8 * k : 8 * k + 8, :] for k in range(z.shape[0] // 8)]
    while len(parts) > 1:
        parts = [a + b for a, b in zip(parts[::2], parts[1::2])]
    fold[...] = parts[0]
    left = fold[0:1, :] + fold[2:3, :] + fold[4:5, :] + fold[6:7, :]
    right = fold[1:2, :] + fold[3:4, :] + fold[5:6, :] + fold[7:8, :]
    columns = [at_lane(left if f < 16 else right, f * HI % LANES) for f in range(N_C)]
    columns += [at_lane(right, E_COL + f * HI) for f in range(CPAR)]
    low6, inv6 = factor(columns[:N_C], CPAR)
    white = forward(low6, inv6, columns[N_C:])
    solved = backward(low6, inv6, white)
    lane = lax.broadcasted_iota(jnp.int32, (1, LANES), 1)
    row = jnp.zeros((1, LANES), F32)
    for j, value in enumerate(white + solved):
        moved = pltpu.roll(value, j * HI, 1) if j else value
        row = jnp.where((lane >= j * HI) & (lane < (j + 1) * HI), moved, row)
    row_out[...] = jnp.broadcast_to(row, row_out.shape)
    glob = [at_lane(right, G_COL + k) for k in range(N_G + GPAR)]
    low4, inv4 = factor(glob[:N_G], GPAR)
    white4 = forward(low4, inv4, glob[N_G:])
    solved4 = backward(low4, inv4, white4)
    for k, value in enumerate(solved4):
        glob_out[k : k + 1, :] = value
    row = white4[0]
    for k in range(1, GPAR):
        row = jnp.where(lane == k, pltpu.roll(white4[k], k, 1), row)
    step_out[...] = row[:, :GPAR]


def final_kernel(table, second, cp, ci, gp, glob, res_out, calib_out, rows):
    for core in range(2):
        held = [table[16 * p + 8 * core : 16 * p + 8 * core + 8, :] for p in range(LO // 16)]
        rows[:, core * LANES : (core + 1) * LANES] = jnp.transpose(jnp.concatenate(held, axis=0))
    for j in range(CPAR):
        for h in range(HI):
            calib_out[j : j + 1, h * LO : (h + 1) * LO] = rows[j * HI + h : j * HI + h + 1, :]
    unit = ci[...]
    row_id = unit >> 7
    lane_id = unit & (LANES - 1)
    picked = [jnp.zeros((TILES, LANES), F32) for _ in range(CPAR)]
    for h in range(2 * HI):
        mine = row_id == h
        half = (h & 1) * LANES
        for c in range(CPAR):
            at = (CPAR + c) * HI + (h >> 1)
            row = jnp.broadcast_to(rows[at : at + 1, half : half + LANES], (TILES, LANES))
            picked[c] = jnp.where(mine, jnp.take_along_axis(row, lane_id, axis=1), picked[c])
    total = cp[0] * picked[0]
    for c in range(1, CPAR):
        total = total + cp[c] * picked[c]
    out = second[...] - total
    shift = gp[0] * glob[0:1, 0:1]
    for a in range(1, GPAR):
        shift = shift + gp[a] * glob[a : a + 1, 0:1]
    res_out[...] = out - shift


NODES = 3072
TM = ("pair", "core")


def paired(x, start):
    count = lax.axis_size(TM)
    low = range(start, count - 1, 2)
    return lax.ppermute(x, TM, [(i, i + 1) for i in low] + [(i + 1, i) for i in low])


def call(kernel, outs, scratch, *args, flops=0, limit=16 << 20, far=False):
    out_shape = [jax.ShapeDtypeStruct(s, d) for s, d in outs]
    vmem = pl.BlockSpec(memory_space=pltpu.VMEM)
    given = pl.BlockSpec(memory_space=pltpu.HBM) if far else vmem
    return pl.pallas_call(
        kernel,
        out_shape=out_shape,
        in_specs=[given] * len(args),
        out_specs=[vmem] * len(outs),
        scratch_shapes=scratch,
        compiler_params=pltpu.CompilerParams(vmem_limit_bytes=limit),
        cost_estimate=pl.CostEstimate(flops=flops, transcendentals=0, bytes_accessed=1 << 20),
    )(*(pltpu.with_memory_space_constraint(a, pltpu.HBM) if far else a for a in args))


def per_device(res, w, sp, si, sd, ap, ph, kn, cp, ci, gp):
    tiles = (TILES, LANES)
    rows = TILES * LANES
    vmem = pltpu.VMEM
    res, w, si, ph, kn, ci = (x.reshape(tiles) for x in (res, w, si, ph, kn, ci))
    sp, ap, cp, gp = (x.reshape(x.shape[0], *tiles) for x in (sp, ap, cp, gp))
    sd = sd.reshape(SPAR, -1, LANES)
    groups = lax.axis_size("grp")
    kept = [(x.shape, x.dtype) for x in (w, ap, ph, kn, cp, ci, gp)]
    first, copies, w, ap, ph, kn, cp, ci, gp = call(
        attitude_kernel,
        [(tiles, F32), ((groups, 32, LANES), F32)] + kept,
        [vmem(x.shape, x.dtype) for x in (res, sp, si, sd)]
        + [
            vmem((60 * TILES, LANES), F32),
            vmem((LANES, rows), BF16),
            vmem((12 * TILES, LANES), F32),
            vmem((32, rows), BF16),
            vmem((LANES, rows), BF16),
            vmem((LANES // 2, LANES), F32),
            vmem((32, LANES), F32),
            pltpu.SemaphoreType.DMA((11,)),
        ],
        w, ap, ph, kn, cp, ci, gp, res, sp, si, sd, flops=1 << 24, far=True,
    )
    gathered = lax.all_to_all(copies, "grp", split_axis=0, concat_axis=0, tiled=True)
    zl, zr, hot = call(
        matrix_kernel,
        [((LO, LANES), F32), ((LO, LANES), F32), ((LO, rows), BF16)],
        [vmem((2, N_C * TILES, LANES), F32), vmem((2 * LANES, rows), BF16), vmem((2 * LANES, rows), BF16)],
        w, cp, ci, gp, kn, flops=1 << 27,
    )
    own = gathered.sum(axis=0)
    outside = paired(own, 1)
    inside = paired(own, 0)
    second, step, keep, send = call(
        sweep_kernel,
        [(tiles, F32), ((3, ND), F32), ((LO, LANES), F32), ((LO, LANES), F32)],
        [vmem((32, LANES), F32), vmem((2, CPAR * TILES, LANES), F32), vmem((LANES, rows), BF16)],
        own, inside, outside, kn, first, ph, ap, w, cp, ci, gp, hot, zl, zr, flops=1 << 24,
    )
    z = (keep + paired(send, 0)).reshape(LO // 2, 2, LANES)
    z = lax.all_to_all(z, ("pair", "grp"), split_axis=0, concat_axis=0, tiled=True)
    copies, glob, glob_step = call(
        solve_kernel,
        [((LO, LANES), F32), ((2 * GPAR, LANES), F32), ((1, GPAR), F32)],
        [vmem((8, LANES), F32)],
        z.reshape(LO, LANES),
    )
    table = lax.all_to_all(copies.reshape(LO, 1, LANES), (*TM, "grp"), split_axis=0, concat_axis=0, tiled=True)
    out, calib = call(
        final_kernel,
        [(tiles, F32), ((CPAR, UNITS), F32)],
        [vmem((LANES, LO), F32)],
        table.reshape(LO, LANES), second, cp, ci, gp, glob,
    )
    return out.reshape(1, 1, rows), step, calib, glob_step.reshape(GPAR)


def solution(mesh):
    count, groups = mesh.devices.shape
    mesh = Mesh(mesh.devices.reshape(count // 2, 2, groups), (*TM, "grp"))
    return jax.shard_map(
        per_device,
        mesh=mesh,
        in_specs=(
            P(TM, "grp", None),
            P(TM, "grp", None),
            P(None, TM, "grp", None),
            P(TM, "grp", None),
            P(None, TM, None),
            P(None, TM, "grp", None),
            P(TM, "grp", None),
            P(TM, "grp", None),
            P(None, TM, "grp", None),
            P(TM, "grp", None),
            P(None, TM, "grp", None),
        ),
        out_specs=(P(TM, "grp", None), P(None, TM), P(), P()),
        check_vma=False,
    )
```

```python
import jax
import jax.numpy as jnp
from jax import lax
from jax.experimental import pallas as pl
from jax.experimental.pallas import tpu as pltpu
from jax.sharding import Mesh
from jax.sharding import PartitionSpec as P

LANES = 128
TILES = 24
KPT = 4
UNITS = 2048
CPAR = 6
GPAR = 4
SPAR = 5
ATT_SWEEPS = 4
ND = 96
HALO = 9
OMEGA = 0.6
RIDGE = 1.0
HI = 8
LO = 256
CHUNK = 8
BAND = 24
F32 = jnp.float32
BF16 = jnp.bfloat16


def pairs(extent):
    return [(a, b) for a in range(extent) for b in range(a, extent)]


PAIR_AT = {extent: {p: i for i, p in enumerate(pairs(extent))} for extent in (3, 4, 6)}


def entry(values, extent, a, b):
    return values[PAIR_AT[extent][(min(a, b), max(a, b))]]


def factor(values, extent):
    low = [[None] * extent for _ in range(extent)]
    inv = [None] * extent
    for c in range(extent):
        pivot = entry(values, extent, c, c) + RIDGE
        for k in range(c):
            pivot = pivot - low[c][k] * low[c][k]
        low[c][c] = jnp.sqrt(pivot)
        inv[c] = 1.0 / low[c][c]
        for r in range(c + 1, extent):
            value = entry(values, extent, r, c)
            for k in range(c):
                value = value - low[r][k] * low[c][k]
            low[r][c] = value * inv[c]
    return low, inv


def forward(low, inv, vector):
    out = []
    for r in range(len(vector)):
        value = vector[r]
        for k in range(r):
            value = value - low[r][k] * out[k]
        out.append(value * inv[r])
    return out


def backward(low, inv, vector):
    extent = len(vector)
    out = [None] * extent
    for r in reversed(range(extent)):
        value = vector[r]
        for k in range(r + 1, extent):
            value = value - low[k][r] * out[k]
        out[r] = value * inv[r]
    return out


def spline(u):
    v = 1.0 - u
    s = u * u
    c = s * u
    sixth = 1.0 / 6.0
    return [
        v * v * v * sixth,
        (3.0 * c - 6.0 * s + 4.0) * sixth,
        (-3.0 * c + 3.0 * s + 3.0 * u + 1.0) * sixth,
        c * sixth,
    ]


def halves(x):
    top = x.astype(BF16).astype(F32)
    return top, x - top


def thirds(x):
    top, rest = halves(x)
    return (top, *halves(rest))


def dot_nt(a, b):
    return lax.dot_general(a, b, (((1,), (1,)), ((), ())), preferred_element_type=F32)


def attitude_kernel(*refs):
    far, refs = refs[:11], refs[11:]
    (first_out, att_out), near, refs = refs[:2], refs[2:9], refs[9:]
    near, refs = (*near, *refs[:4]), refs[4:]
    feat, lhs, rhs_feat, rhs, hot, acc, shut, sems = refs
    loads = [pltpu.make_async_copy(a, b, sems.at[i]) for i, (a, b) in enumerate(zip(far, near))]
    for i in (10, 9, 0, 1, 2, 3, 8, 7, 4, 5, 6):
        loads[i].start()
    w, ap, ph, kn, cp, ci, gp, res, sp, si, sd = near
    for i in (10, 9, 0, 1, 2, 3, 8, 7):
        loads[i].wait()
    basis = spline(ph[...])
    weight = w[...]
    att = [ap[a] for a in range(3)]
    outer = [weight * att[a] * att[b] for a, b in pairs(3)]
    at = 0
    for i in range(4):
        for d in range(4 - i):
            both = basis[i] * basis[i + d]
            for value in outer:
                feat[pl.ds(at * TILES, TILES), :] = both * value
                at += 1
    count = at
    node = lax.broadcasted_iota(jnp.int32, (LANES, LANES), 0)
    index = si[...]
    row_id = index >> 7
    lane_id = index & (LANES - 1)
    picked = [jnp.zeros((TILES, LANES), F32) for _ in range(SPAR)]
    half = lhs.shape[0] // 2
    band = None
    steps = TILES // CHUNK
    for s in range(steps):
        for t in range(s * CHUNK, (s + 1) * CHUNK):
            cols = slice(t * LANES, (t + 1) * LANES)
            top, low = halves(feat[pl.ds(t, count, stride=TILES), :])
            lhs[0:count, cols] = top.astype(BF16)
            lhs[half : half + count, cols] = low.astype(BF16)
            slot = (kn[t : t + 1, :] & (KPT - 1)) + (KPT * t + HALO)
            hot[:, cols] = jnp.where(node == slot, 1.0, 0.0).astype(BF16)
        cols = slice(s * CHUNK * LANES, (s + 1) * CHUNK * LANES)
        part = dot_nt(lhs[:, cols], hot[:, cols])
        band = part if band is None else band + part
        for h in range(s * sd.shape[1] // steps, (s + 1) * sd.shape[1] // steps):
            mine = row_id == h
            for c in range(SPAR):
                row = jnp.broadcast_to(sd[c, h : h + 1, :], (TILES, LANES))
                picked[c] = jnp.where(mine, jnp.take_along_axis(row, lane_id, axis=1), picked[c])
    acc[...] = band[:half] + band[half:]
    total = sp[0] * picked[0]
    for c in range(1, SPAR):
        total = total + sp[c] * picked[c]
    first = res[...] - total
    first_out[...] = first
    at = 0
    for i in range(4):
        for a in range(3):
            rhs_feat[pl.ds(at * TILES, TILES), :] = basis[i] * (weight * att[a] * first)
            at += 1
    for t in range(TILES):
        cols = slice(t * LANES, (t + 1) * LANES)
        for k, part in enumerate(thirds(rhs_feat[pl.ds(t, at, stride=TILES), :])):
            rhs[16 * k : 16 * k + at, cols] = part.astype(BF16)
    both = dot_nt(rhs[...], hot[...])
    both = both[:16] + (both[16:32] + both[32:])
    shut[...] = jnp.zeros_like(shut)
    at = 0
    side = both[0:3]
    for i in range(4):
        rows = 6 * (4 - i)
        value = acc[at : at + rows, :]
        if i:
            value = pltpu.roll(value, i, 1)
            side = side + pltpu.roll(both[3 * i : 3 * i + 3, :], i, 1)
        shut[0:rows, :] = shut[0:rows, :] + value
        at += rows
    shut[BAND : BAND + 3, :] = side
    att_out[...] = jnp.broadcast_to(shut[...][None], att_out.shape)
    for i in (4, 5, 6):
        loads[i].wait()


def unit_hot(unit, flip, hot):
    lo_id = lax.broadcasted_iota(jnp.int32, (LO, LANES), 0)
    for t in range(TILES):
        cols = slice(t * LANES, (t + 1) * LANES)
        lo = (unit[t : t + 1, :] & (LO - 1)) ^ flip
        hot[:, cols] = jnp.where(lo_id == lo, 1.0, 0.0).astype(BF16)


def spread(unit, feats, parts, split, *places):
    for f, value in enumerate(feats):
        for k, part in enumerate(split(value)):
            parts[k, pl.ds(f * TILES, TILES), :] = part
    hi_id = lax.broadcasted_iota(jnp.int32, (HI, LANES), 0)
    zero = jnp.zeros((HI, LANES), F32)
    for t in range(TILES):
        cols = slice(t * LANES, (t + 1) * LANES)
        mine = hi_id == (unit[t : t + 1, :] >> 8)
        for part, (to, base) in enumerate(places):
            for f in range(0, len(feats), 2):
                rows = []
                for g in (f, f + 1):
                    if g < len(feats):
                        row = parts[part, g * TILES + t : g * TILES + t + 1, :]
                        rows.append(jnp.where(mine, jnp.broadcast_to(row, (HI, LANES)), 0.0))
                    else:
                        rows.append(zero)
                at = base + f * HI
                to[at : at + 2 * HI, cols] = jnp.concatenate(rows, axis=0).astype(BF16)


def totals_row(values, first_lane):
    lane = lax.broadcasted_iota(jnp.int32, (1, LANES), 1)
    row = jnp.zeros((1, LANES), F32)
    for k, value in enumerate(values):
        folded = value[0:8] + value[8:16] + value[16:24]
        total = jnp.sum(jnp.sum(folded, axis=1, keepdims=True), axis=0, keepdims=True)
        row = jnp.where(lane == first_lane + k, total, row)
    return row


N_C = CPAR * (CPAR + 1) // 2
N_G = GPAR * (GPAR + 1) // 2
E_COL = (N_C + 1) // 2 * 2 * HI - LANES
G_COL = E_COL + CPAR * HI
H_COL = G_COL + N_G


def matrix_kernel(w, cp, ci, gp, kn, left_out, right_out, hot_out, parts, top, low):
    weight = w[...]
    calib = [cp[a] for a in range(CPAR)]
    weighted = [weight * c for c in calib]
    feats = [weighted[a] * calib[b] for a, b in pairs(CPAR)]
    used = (N_C + 1) // 2 * 2 * HI
    top[used:, :] = jnp.zeros((2 * LANES - used, top.shape[1]), BF16)
    low[used:, :] = jnp.zeros((2 * LANES - used, top.shape[1]), BF16)
    spread(ci, feats, parts, halves, (top, 0), (low, 0))
    flip = ((kn[0:1, 0:1] >> 5) & 1) << 7
    unit_hot(ci, jnp.broadcast_to(flip, (1, LANES)), hot_out)
    hot = hot_out[...]
    both = dot_nt(hot, top[...]) + dot_nt(hot, low[...])
    glob = [gp[a] for a in range(GPAR)]
    sums = totals_row([weight * glob[a] * glob[b] for a, b in pairs(GPAR)], G_COL)
    left_out[...] = both[:, :LANES]
    right_out[...] = both[:, LANES:] + sums


def sweep_kernel(
    own, inside, outside, kn, first_in, ph, ap, w, cp, ci, gp, hot, zl, zr, second_out, step_out, keep_out, send_out, ext, parts, mid
):
    lane = lax.broadcasted_iota(jnp.int32, own.shape, 1)
    base = jnp.broadcast_to(kn[0:1, 0:1] & ~(KPT - 1), (1, LANES))
    odd = ((base >> 5) & 1) == 1
    left = jnp.where(odd, inside[...], outside[...])
    right = jnp.where(odd, outside[...], inside[...])
    at_left = lane < HALO + 3
    at_right = (lane >= HALO + ND) & (lane < HALO + ND + 12)
    ext[...] = (
        own[...]
        + jnp.where(at_left, pltpu.roll(left, LANES - ND, 1), 0.0)
        + jnp.where(at_right, pltpu.roll(right, ND, 1), 0.0)
    )
    row = [ext[r : r + 1, :] for r in range(BAND + 3)]
    node = base + lax.broadcasted_iota(jnp.int32, (1, LANES), 1) - HALO
    exists = (node >= 0) & (node < NODES)
    rhs = row[BAND:]
    band = [row[6 * d : 6 * d + 6] for d in range(4)]
    low3, inv3 = factor(band[0], 3)

    def precondition(vector):
        return [OMEGA * v for v in backward(low3, inv3, forward(low3, inv3, vector))]

    def times(values, x, a):
        out = entry(values, 3, a, 0) * x[0]
        out = out + entry(values, 3, a, 1) * x[1]
        return out + entry(values, 3, a, 2) * x[2]

    def kept(values):
        return [jnp.where(exists, v, 0.0) for v in values]

    x = kept(precondition(rhs))
    for _ in range(1, ATT_SWEEPS):
        rest = [rhs[a] - x[a] - times(band[0], x, a) for a in range(3)]
        for d in range(1, 4):
            ahead = [pltpu.roll(v, LANES - d, 1) for v in x]
            for a in range(3):
                rest[a] = rest[a] - times(band[d], ahead, a)
                rest[a] = rest[a] - pltpu.roll(times(band[d], x, a), d, 1)
        step = precondition(rest)
        x = kept([x[a] + step[a] for a in range(3)])
    for c in range(3):
        value = low3[c][c] * x[c]
        for k in range(c + 1, 3):
            value = value + low3[k][c] * x[k]
        step_out[c : c + 1, :] = pltpu.roll(value, LANES - HALO, 1)[:, :ND]
    tile = lax.broadcasted_iota(jnp.int32, (TILES, LANES), 0)
    local = (kn[...] & (KPT - 1)) + KPT * tile + HALO
    basis = spline(ph[...])
    att = [ap[a] for a in range(3)]
    spread_x = [jnp.broadcast_to(v, (TILES, LANES)) for v in x]
    second = first_in[...]
    for i in range(4):
        dot = att[0] * jnp.take_along_axis(spread_x[0], local + i, axis=1)
        for a in range(1, 3):
            dot = dot + att[a] * jnp.take_along_axis(spread_x[a], local + i, axis=1)
        second = second - basis[i] * dot
    second_out[...] = second
    push = w[...] * second
    feats = [push * cp[a] for a in range(CPAR)]
    span = CPAR * HI
    spread(ci, feats, parts, thirds, *((mid, k * span) for k in range(3)))
    both = dot_nt(mid[...], hot[...])
    both = both[:span] + (both[span : 2 * span] + both[2 * span :])
    above = jnp.zeros((E_COL, LO), F32)
    below = jnp.zeros((LANES - G_COL, LO), F32)
    both = jnp.concatenate([above, both, below], axis=0)
    both = jnp.concatenate([jnp.transpose(both[:, :LANES]), jnp.transpose(both[:, LANES:])], axis=0)
    sums = totals_row([push * gp[a] for a in range(GPAR)], H_COL)
    right = zr[...] + both + sums
    for to, at in ((keep_out, 0), (send_out, LO // 2)):
        to[pl.ds(0, LO // 2, stride=2), :] = zl[at : at + LO // 2, :]
        to[pl.ds(1, LO // 2, stride=2), :] = right[at : at + LO // 2, :]


def at_lane(row, start):
    return pltpu.roll(row, (LANES - start) % LANES, 1) if start else row


def solve_kernel(z, row_out, glob_out, step_out, fold):
    parts = [z[8 * k : 8 * k + 8, :] for k in range(z.shape[0] // 8)]
    while len(parts) > 1:
        parts = [a + b for a, b in zip(parts[::2], parts[1::2])]
    fold[...] = parts[0]
    left = fold[0:1, :] + fold[2:3, :] + fold[4:5, :] + fold[6:7, :]
    right = fold[1:2, :] + fold[3:4, :] + fold[5:6, :] + fold[7:8, :]
    columns = [at_lane(left if f < 16 else right, f * HI % LANES) for f in range(N_C)]
    columns += [at_lane(right, E_COL + f * HI) for f in range(CPAR)]
    low6, inv6 = factor(columns[:N_C], CPAR)
    white = forward(low6, inv6, columns[N_C:])
    solved = backward(low6, inv6, white)
    lane = lax.broadcasted_iota(jnp.int32, (1, LANES), 1)
    row = jnp.zeros((1, LANES), F32)
    for j, value in enumerate(white + solved):
        moved = pltpu.roll(value, j * HI, 1) if j else value
        row = jnp.where((lane >= j * HI) & (lane < (j + 1) * HI), moved, row)
    row_out[...] = jnp.broadcast_to(row, row_out.shape)
    glob = [at_lane(right, G_COL + k) for k in range(N_G + GPAR)]
    low4, inv4 = factor(glob[:N_G], GPAR)
    white4 = forward(low4, inv4, glob[N_G:])
    solved4 = backward(low4, inv4, white4)
    for k, value in enumerate(solved4):
        glob_out[k : k + 1, :] = value
    row = white4[0]
    for k in range(1, GPAR):
        row = jnp.where(lane == k, pltpu.roll(white4[k], k, 1), row)
    step_out[...] = row[:, :GPAR]


def final_kernel(table, second, cp, ci, gp, glob, res_out, calib_out, rows):
    for core in range(2):
        held = [table[16 * p + 8 * core : 16 * p + 8 * core + 8, :] for p in range(LO // 16)]
        rows[:, core * LANES : (core + 1) * LANES] = jnp.transpose(jnp.concatenate(held, axis=0))
    for j in range(CPAR):
        for h in range(HI):
            calib_out[j : j + 1, h * LO : (h + 1) * LO] = rows[j * HI + h : j * HI + h + 1, :]
    unit = ci[...]
    row_id = unit >> 7
    lane_id = unit & (LANES - 1)
    picked = [jnp.zeros((TILES, LANES), F32) for _ in range(CPAR)]
    for h in range(2 * HI):
        mine = row_id == h
        half = (h & 1) * LANES
        for c in range(CPAR):
            at = (CPAR + c) * HI + (h >> 1)
            row = jnp.broadcast_to(rows[at : at + 1, half : half + LANES], (TILES, LANES))
            picked[c] = jnp.where(mine, jnp.take_along_axis(row, lane_id, axis=1), picked[c])
    total = cp[0] * picked[0]
    for c in range(1, CPAR):
        total = total + cp[c] * picked[c]
    out = second[...] - total
    shift = gp[0] * glob[0:1, 0:1]
    for a in range(1, GPAR):
        shift = shift + gp[a] * glob[a : a + 1, 0:1]
    res_out[...] = out - shift


NODES = 3072
TM = ("pair", "core")


def paired(x, start):
    count = lax.axis_size(TM)
    low = range(start, count - 1, 2)
    return lax.ppermute(x, TM, [(i, i + 1) for i in low] + [(i + 1, i) for i in low])


def call(kernel, outs, scratch, *args, flops=0, limit=16 << 20, far=False):
    out_shape = [jax.ShapeDtypeStruct(s, d) for s, d in outs]
    vmem = pl.BlockSpec(memory_space=pltpu.VMEM)
    given = pl.BlockSpec(memory_space=pltpu.HBM) if far else vmem
    return pl.pallas_call(
        kernel,
        out_shape=out_shape,
        in_specs=[given] * len(args),
        out_specs=[vmem] * len(outs),
        scratch_shapes=scratch,
        compiler_params=pltpu.CompilerParams(vmem_limit_bytes=limit),
        cost_estimate=pl.CostEstimate(flops=flops, transcendentals=0, bytes_accessed=1 << 20),
    )(*(pltpu.with_memory_space_constraint(a, pltpu.HBM) if far else a for a in args))


def per_device(res, w, sp, si, sd, ap, ph, kn, cp, ci, gp):
    tiles = (TILES, LANES)
    rows = TILES * LANES
    vmem = pltpu.VMEM
    res, w, si, ph, kn, ci = (x.reshape(tiles) for x in (res, w, si, ph, kn, ci))
    sp, ap, cp, gp = (x.reshape(x.shape[0], *tiles) for x in (sp, ap, cp, gp))
    sd = sd.reshape(SPAR, -1, LANES)
    groups = lax.axis_size("grp")
    kept = [(x.shape, x.dtype) for x in (w, ap, ph, kn, cp, ci, gp)]
    first, copies, w, ap, ph, kn, cp, ci, gp = call(
        attitude_kernel,
        [(tiles, F32), ((groups, 32, LANES), F32)] + kept,
        [vmem(x.shape, x.dtype) for x in (res, sp, si, sd)]
        + [
            vmem((60 * TILES, LANES), F32),
            vmem((LANES, rows), BF16),
            vmem((12 * TILES, LANES), F32),
            vmem((48, rows), BF16),
            vmem((LANES, rows), BF16),
            vmem((LANES // 2, LANES), F32),
            vmem((32, LANES), F32),
            pltpu.SemaphoreType.DMA((11,)),
        ],
        w, ap, ph, kn, cp, ci, gp, res, sp, si, sd, flops=1 << 24, far=True,
    )
    gathered = lax.all_to_all(copies, "grp", split_axis=0, concat_axis=0, tiled=True)
    zl, zr, hot = call(
        matrix_kernel,
        [((LO, LANES), F32), ((LO, LANES), F32), ((LO, rows), BF16)],
        [vmem((2, N_C * TILES, LANES), F32), vmem((2 * LANES, rows), BF16), vmem((2 * LANES, rows), BF16)],
        w, cp, ci, gp, kn, flops=1 << 27,
    )
    own = gathered.sum(axis=0)
    outside = paired(own, 1)
    inside = paired(own, 0)
    second, step, keep, send = call(
        sweep_kernel,
        [(tiles, F32), ((3, ND), F32), ((LO, LANES), F32), ((LO, LANES), F32)],
        [vmem((32, LANES), F32), vmem((3, CPAR * TILES, LANES), F32), vmem((3 * CPAR * HI, rows), BF16)],
        own, inside, outside, kn, first, ph, ap, w, cp, ci, gp, hot, zl, zr, flops=1 << 24,
    )
    z = (keep + paired(send, 0)).reshape(LO // 2, 2, LANES)
    z = lax.all_to_all(z, ("pair", "grp"), split_axis=0, concat_axis=0, tiled=True)
    copies, glob, glob_step = call(
        solve_kernel,
        [((LO, LANES), F32), ((2 * GPAR, LANES), F32), ((1, GPAR), F32)],
        [vmem((8, LANES), F32)],
        z.reshape(LO, LANES),
    )
    table = lax.all_to_all(copies.reshape(LO, 1, LANES), (*TM, "grp"), split_axis=0, concat_axis=0, tiled=True)
    out, calib = call(
        final_kernel,
        [(tiles, F32), ((CPAR, UNITS), F32)],
        [vmem((LANES, LO), F32)],
        table.reshape(LO, LANES), second, cp, ci, gp, glob,
    )
    return out.reshape(1, 1, rows), step, calib, glob_step.reshape(GPAR)


def solution(mesh):
    count, groups = mesh.devices.shape
    mesh = Mesh(mesh.devices.reshape(count // 2, 2, groups), (*TM, "grp"))
    return jax.shard_map(
        per_device,
        mesh=mesh,
        in_specs=(
            P(TM, "grp", None),
            P(TM, "grp", None),
            P(None, TM, "grp", None),
            P(TM, "grp", None),
            P(None, TM, None),
            P(None, TM, "grp", None),
            P(TM, "grp", None),
            P(TM, "grp", None),
            P(None, TM, "grp", None),
            P(TM, "grp", None),
            P(None, TM, "grp", None),
        ),
        out_specs=(P(TM, "grp", None), P(None, TM), P(), P()),
        check_vma=False,
    )
```

```python
import jax
import jax.numpy as jnp
from jax import lax
from jax.experimental import pallas as pl
from jax.experimental.pallas import tpu as pltpu
from jax.sharding import Mesh
from jax.sharding import PartitionSpec as P

LANES = 128
TILES = 24
KPT = 4
UNITS = 2048
CPAR = 6
GPAR = 4
SPAR = 5
ATT_SWEEPS = 4
ND = 96
HALO = 9
OMEGA = 0.6
RIDGE = 1.0
HI = 8
LO = 256
CHUNK = 8
BAND = 24
F32 = jnp.float32
BF16 = jnp.bfloat16


def pairs(extent):
    return [(a, b) for a in range(extent) for b in range(a, extent)]


PAIR_AT = {extent: {p: i for i, p in enumerate(pairs(extent))} for extent in (3, 4, 6)}


def entry(values, extent, a, b):
    return values[PAIR_AT[extent][(min(a, b), max(a, b))]]


def factor(values, extent):
    low = [[None] * extent for _ in range(extent)]
    inv = [None] * extent
    for c in range(extent):
        pivot = entry(values, extent, c, c) + RIDGE
        for k in range(c):
            pivot = pivot - low[c][k] * low[c][k]
        inv[c] = lax.rsqrt(pivot)
        low[c][c] = pivot * inv[c]
        for r in range(c + 1, extent):
            value = entry(values, extent, r, c)
            for k in range(c):
                value = value - low[r][k] * low[c][k]
            low[r][c] = value * inv[c]
    return low, inv


def forward(low, inv, vector):
    out = []
    for r in range(len(vector)):
        value = vector[r]
        for k in range(r):
            value = value - low[r][k] * out[k]
        out.append(value * inv[r])
    return out


def backward(low, inv, vector):
    extent = len(vector)
    out = [None] * extent
    for r in reversed(range(extent)):
        value = vector[r]
        for k in range(r + 1, extent):
            value = value - low[k][r] * out[k]
        out[r] = value * inv[r]
    return out


def spline(u):
    v = 1.0 - u
    s = u * u
    c = s * u
    sixth = 1.0 / 6.0
    return [
        v * v * v * sixth,
        (3.0 * c - 6.0 * s + 4.0) * sixth,
        (-3.0 * c + 3.0 * s + 3.0 * u + 1.0) * sixth,
        c * sixth,
    ]


def halves(x):
    top = x.astype(BF16).astype(F32)
    return top, x - top


def thirds(x):
    top, rest = halves(x)
    return (top, *halves(rest))


def dot_nt(a, b):
    return lax.dot_general(a, b, (((1,), (1,)), ((), ())), preferred_element_type=F32)


def attitude_kernel(*refs):
    far, refs = refs[:11], refs[11:]
    (first_out, att_out), near, refs = refs[:2], refs[2:9], refs[9:]
    near, refs = (*near, *refs[:4]), refs[4:]
    feat, lhs, rhs_feat, rhs, hot, acc, shut, sems = refs
    loads = [pltpu.make_async_copy(a, b, sems.at[i]) for i, (a, b) in enumerate(zip(far, near))]
    for i in (10, 9, 0, 1, 2, 3, 8, 7, 4, 5, 6):
        loads[i].start()
    w, ap, ph, kn, cp, ci, gp, res, sp, si, sd = near
    for i in (10, 9, 0, 1, 2, 3, 8, 7):
        loads[i].wait()
    basis = spline(ph[...])
    weight = w[...]
    att = [ap[a] for a in range(3)]
    outer = [weight * att[a] * att[b] for a, b in pairs(3)]
    at = 0
    for i in range(4):
        for d in range(4 - i):
            both = basis[i] * basis[i + d]
            for value in outer:
                feat[pl.ds(at * TILES, TILES), :] = both * value
                at += 1
    count = at
    node = lax.broadcasted_iota(jnp.int32, (LANES, LANES), 0)
    index = si[...]
    row_id = index >> 7
    lane_id = index & (LANES - 1)
    picked = [jnp.zeros((TILES, LANES), F32) for _ in range(SPAR)]
    half = lhs.shape[0] // 2
    band = None
    steps = TILES // CHUNK
    for s in range(steps):
        for t in range(s * CHUNK, (s + 1) * CHUNK):
            cols = slice(t * LANES, (t + 1) * LANES)
            top, low = halves(feat[pl.ds(t, count, stride=TILES), :])
            lhs[0:count, cols] = top.astype(BF16)
            lhs[half : half + count, cols] = low.astype(BF16)
            slot = (kn[t : t + 1, :] & (KPT - 1)) + (KPT * t + HALO)
            hot[:, cols] = jnp.where(node == slot, 1.0, 0.0).astype(BF16)
        cols = slice(s * CHUNK * LANES, (s + 1) * CHUNK * LANES)
        part = dot_nt(lhs[:, cols], hot[:, cols])
        band = part if band is None else band + part
        for h in range(s * sd.shape[1] // steps, (s + 1) * sd.shape[1] // steps):
            mine = row_id == h
            for c in range(SPAR):
                row = jnp.broadcast_to(sd[c, h : h + 1, :], (TILES, LANES))
                picked[c] = jnp.where(mine, jnp.take_along_axis(row, lane_id, axis=1), picked[c])
    acc[...] = band[:half] + band[half:]
    total = sp[0] * picked[0]
    for c in range(1, SPAR):
        total = total + sp[c] * picked[c]
    first = res[...] - total
    first_out[...] = first
    at = 0
    for i in range(4):
        for a in range(3):
            rhs_feat[pl.ds(at * TILES, TILES), :] = basis[i] * (weight * att[a] * first)
            at += 1
    for t in range(TILES):
        cols = slice(t * LANES, (t + 1) * LANES)
        for k, part in enumerate(thirds(rhs_feat[pl.ds(t, at, stride=TILES), :])):
            rhs[16 * k : 16 * k + at, cols] = part.astype(BF16)
    both = dot_nt(rhs[...], hot[...])
    both = both[:16] + (both[16:32] + both[32:])
    shut[...] = jnp.zeros_like(shut)
    at = 0
    side = both[0:3]
    for i in range(4):
        rows = 6 * (4 - i)
        value = acc[at : at + rows, :]
        if i:
            value = pltpu.roll(value, i, 1)
            side = side + pltpu.roll(both[3 * i : 3 * i + 3, :], i, 1)
        shut[0:rows, :] = shut[0:rows, :] + value
        at += rows
    shut[BAND : BAND + 3, :] = side
    att_out[...] = jnp.broadcast_to(shut[...][None], att_out.shape)
    for i in (4, 5, 6):
        loads[i].wait()


def unit_hot(unit, flip, hot):
    lo_id = lax.broadcasted_iota(jnp.int32, (LO, LANES), 0)
    for t in range(TILES):
        cols = slice(t * LANES, (t + 1) * LANES)
        lo = (unit[t : t + 1, :] & (LO - 1)) ^ flip
        hot[:, cols] = jnp.where(lo_id == lo, 1.0, 0.0).astype(BF16)


def spread(unit, feats, parts, split, *places):
    for f, value in enumerate(feats):
        for k, part in enumerate(split(value)):
            parts[k, pl.ds(f * TILES, TILES), :] = part
    hi_id = lax.broadcasted_iota(jnp.int32, (HI, LANES), 0)
    zero = jnp.zeros((HI, LANES), F32)
    for t in range(TILES):
        cols = slice(t * LANES, (t + 1) * LANES)
        mine = hi_id == (unit[t : t + 1, :] >> 8)
        for part, (to, base) in enumerate(places):
            for f in range(0, len(feats), 2):
                rows = []
                for g in (f, f + 1):
                    if g < len(feats):
                        row = parts[part, g * TILES + t : g * TILES + t + 1, :]
                        rows.append(jnp.where(mine, jnp.broadcast_to(row, (HI, LANES)), 0.0))
                    else:
                        rows.append(zero)
                at = base + f * HI
                to[at : at + 2 * HI, cols] = jnp.concatenate(rows, axis=0).astype(BF16)


def totals_row(values, first_lane):
    lane = lax.broadcasted_iota(jnp.int32, (1, LANES), 1)
    row = jnp.zeros((1, LANES), F32)
    for k, value in enumerate(values):
        folded = value[0:8] + value[8:16] + value[16:24]
        total = jnp.sum(jnp.sum(folded, axis=1, keepdims=True), axis=0, keepdims=True)
        row = jnp.where(lane == first_lane + k, total, row)
    return row


N_C = CPAR * (CPAR + 1) // 2
N_G = GPAR * (GPAR + 1) // 2
E_COL = (N_C + 1) // 2 * 2 * HI - LANES
G_COL = E_COL + CPAR * HI
H_COL = G_COL + N_G


def matrix_kernel(w, cp, ci, gp, kn, left_out, right_out, hot_out, parts, top, low):
    weight = w[...]
    calib = [cp[a] for a in range(CPAR)]
    weighted = [weight * c for c in calib]
    feats = [weighted[a] * calib[b] for a, b in pairs(CPAR)]
    used = (N_C + 1) // 2 * 2 * HI
    top[used:, :] = jnp.zeros((2 * LANES - used, top.shape[1]), BF16)
    low[used:, :] = jnp.zeros((2 * LANES - used, top.shape[1]), BF16)
    spread(ci, feats, parts, halves, (top, 0), (low, 0))
    flip = ((kn[0:1, 0:1] >> 5) & 1) << 7
    unit_hot(ci, jnp.broadcast_to(flip, (1, LANES)), hot_out)
    hot = hot_out[...]
    both = dot_nt(hot, top[...]) + dot_nt(hot, low[...])
    glob = [gp[a] for a in range(GPAR)]
    sums = totals_row([weight * glob[a] * glob[b] for a, b in pairs(GPAR)], G_COL)
    left_out[...] = both[:, :LANES]
    right_out[...] = both[:, LANES:] + sums


def sweep_kernel(
    own, inside, outside, kn, first_in, ph, ap, w, cp, ci, gp, hot, zl, zr, second_out, step_out, keep_out, send_out, ext, parts, mid
):
    lane = lax.broadcasted_iota(jnp.int32, own.shape, 1)
    base = jnp.broadcast_to(kn[0:1, 0:1] & ~(KPT - 1), (1, LANES))
    odd = ((base >> 5) & 1) == 1
    left = jnp.where(odd, inside[...], outside[...])
    right = jnp.where(odd, outside[...], inside[...])
    at_left = lane < HALO + 3
    at_right = (lane >= HALO + ND) & (lane < HALO + ND + 12)
    ext[...] = (
        own[...]
        + jnp.where(at_left, pltpu.roll(left, LANES - ND, 1), 0.0)
        + jnp.where(at_right, pltpu.roll(right, ND, 1), 0.0)
    )
    row = [ext[r : r + 1, :] for r in range(BAND + 3)]
    node = base + lax.broadcasted_iota(jnp.int32, (1, LANES), 1) - HALO
    exists = (node >= 0) & (node < NODES)
    rhs = row[BAND:]
    band = [row[6 * d : 6 * d + 6] for d in range(4)]
    low3, inv3 = factor(band[0], 3)

    def precondition(vector):
        return [OMEGA * v for v in backward(low3, inv3, forward(low3, inv3, vector))]

    def times(values, x, a):
        out = entry(values, 3, a, 0) * x[0]
        out = out + entry(values, 3, a, 1) * x[1]
        return out + entry(values, 3, a, 2) * x[2]

    def kept(values):
        return [jnp.where(exists, v, 0.0) for v in values]

    x = kept(precondition(rhs))
    for _ in range(1, ATT_SWEEPS):
        rest = [rhs[a] - x[a] - times(band[0], x, a) for a in range(3)]
        for d in range(1, 4):
            ahead = [pltpu.roll(v, LANES - d, 1) for v in x]
            for a in range(3):
                rest[a] = rest[a] - times(band[d], ahead, a)
                rest[a] = rest[a] - pltpu.roll(times(band[d], x, a), d, 1)
        step = precondition(rest)
        x = kept([x[a] + step[a] for a in range(3)])
    for c in range(3):
        value = low3[c][c] * x[c]
        for k in range(c + 1, 3):
            value = value + low3[k][c] * x[k]
        step_out[c : c + 1, :] = pltpu.roll(value, LANES - HALO, 1)[:, :ND]
    tile = lax.broadcasted_iota(jnp.int32, (TILES, LANES), 0)
    local = (kn[...] & (KPT - 1)) + KPT * tile + HALO
    basis = spline(ph[...])
    att = [ap[a] for a in range(3)]
    spread_x = [jnp.broadcast_to(v, (TILES, LANES)) for v in x]
    second = first_in[...]
    for i in range(4):
        dot = att[0] * jnp.take_along_axis(spread_x[0], local + i, axis=1)
        for a in range(1, 3):
            dot = dot + att[a] * jnp.take_along_axis(spread_x[a], local + i, axis=1)
        second = second - basis[i] * dot
    second_out[...] = second
    push = w[...] * second
    feats = [push * cp[a] for a in range(CPAR)]
    span = CPAR * HI
    spread(ci, feats, parts, thirds, *((mid, k * span) for k in range(3)))
    both = dot_nt(mid[...], hot[...])
    both = both[:span] + (both[span : 2 * span] + both[2 * span :])
    above = jnp.zeros((E_COL, LO), F32)
    below = jnp.zeros((LANES - G_COL, LO), F32)
    both = jnp.concatenate([above, both, below], axis=0)
    both = jnp.concatenate([jnp.transpose(both[:, :LANES]), jnp.transpose(both[:, LANES:])], axis=0)
    sums = totals_row([push * gp[a] for a in range(GPAR)], H_COL)
    right = zr[...] + both + sums
    for to, at in ((keep_out, 0), (send_out, LO // 2)):
        to[pl.ds(0, LO // 2, stride=2), :] = zl[at : at + LO // 2, :]
        to[pl.ds(1, LO // 2, stride=2), :] = right[at : at + LO // 2, :]


def at_lane(row, start):
    return pltpu.roll(row, (LANES - start) % LANES, 1) if start else row


def solve_kernel(z, row_out, glob_out, step_out, fold):
    parts = [z[8 * k : 8 * k + 8, :] for k in range(z.shape[0] // 8)]
    while len(parts) > 1:
        parts = [a + b for a, b in zip(parts[::2], parts[1::2])]
    fold[...] = parts[0]
    left = fold[0:1, :] + fold[2:3, :] + fold[4:5, :] + fold[6:7, :]
    right = fold[1:2, :] + fold[3:4, :] + fold[5:6, :] + fold[7:8, :]
    columns = [at_lane(left if f < 16 else right, f * HI % LANES) for f in range(N_C)]
    columns += [at_lane(right, E_COL + f * HI) for f in range(CPAR)]
    low6, inv6 = factor(columns[:N_C], CPAR)
    white = forward(low6, inv6, columns[N_C:])
    solved = backward(low6, inv6, white)
    lane = lax.broadcasted_iota(jnp.int32, (1, LANES), 1)
    row = jnp.zeros((1, LANES), F32)
    for j, value in enumerate(white + solved):
        moved = pltpu.roll(value, j * HI, 1) if j else value
        row = jnp.where((lane >= j * HI) & (lane < (j + 1) * HI), moved, row)
    row_out[...] = jnp.broadcast_to(row, row_out.shape)
    glob = [at_lane(right, G_COL + k) for k in range(N_G + GPAR)]
    low4, inv4 = factor(glob[:N_G], GPAR)
    white4 = forward(low4, inv4, glob[N_G:])
    solved4 = backward(low4, inv4, white4)
    for k, value in enumerate(solved4):
        glob_out[k : k + 1, :] = value
    row = white4[0]
    for k in range(1, GPAR):
        row = jnp.where(lane == k, pltpu.roll(white4[k], k, 1), row)
    step_out[...] = row[:, :GPAR]


def final_kernel(table, second, cp, ci, gp, glob, res_out, calib_out, rows):
    for core in range(2):
        held = [table[16 * p + 8 * core : 16 * p + 8 * core + 8, :] for p in range(LO // 16)]
        rows[:, core * LANES : (core + 1) * LANES] = jnp.transpose(jnp.concatenate(held, axis=0))
    for j in range(CPAR):
        for h in range(HI):
            calib_out[j : j + 1, h * LO : (h + 1) * LO] = rows[j * HI + h : j * HI + h + 1, :]
    unit = ci[...]
    row_id = unit >> 7
    lane_id = unit & (LANES - 1)
    picked = [jnp.zeros((TILES, LANES), F32) for _ in range(CPAR)]
    for h in range(2 * HI):
        mine = row_id == h
        half = (h & 1) * LANES
        for c in range(CPAR):
            at = (CPAR + c) * HI + (h >> 1)
            row = jnp.broadcast_to(rows[at : at + 1, half : half + LANES], (TILES, LANES))
            picked[c] = jnp.where(mine, jnp.take_along_axis(row, lane_id, axis=1), picked[c])
    total = cp[0] * picked[0]
    for c in range(1, CPAR):
        total = total + cp[c] * picked[c]
    out = second[...] - total
    shift = gp[0] * glob[0:1, 0:1]
    for a in range(1, GPAR):
        shift = shift + gp[a] * glob[a : a + 1, 0:1]
    res_out[...] = out - shift


NODES = 3072
TM = ("pair", "core")


def paired(x, start):
    count = lax.axis_size(TM)
    low = range(start, count - 1, 2)
    return lax.ppermute(x, TM, [(i, i + 1) for i in low] + [(i + 1, i) for i in low])


def call(kernel, outs, scratch, *args, flops=0, limit=16 << 20, far=False):
    out_shape = [jax.ShapeDtypeStruct(s, d) for s, d in outs]
    vmem = pl.BlockSpec(memory_space=pltpu.VMEM)
    given = pl.BlockSpec(memory_space=pltpu.HBM) if far else vmem
    return pl.pallas_call(
        kernel,
        out_shape=out_shape,
        in_specs=[given] * len(args),
        out_specs=[vmem] * len(outs),
        scratch_shapes=scratch,
        compiler_params=pltpu.CompilerParams(vmem_limit_bytes=limit),
        cost_estimate=pl.CostEstimate(flops=flops, transcendentals=0, bytes_accessed=1 << 20),
    )(*(pltpu.with_memory_space_constraint(a, pltpu.HBM) if far else a for a in args))


def per_device(res, w, sp, si, sd, ap, ph, kn, cp, ci, gp):
    tiles = (TILES, LANES)
    rows = TILES * LANES
    vmem = pltpu.VMEM
    res, w, si, ph, kn, ci = (x.reshape(tiles) for x in (res, w, si, ph, kn, ci))
    sp, ap, cp, gp = (x.reshape(x.shape[0], *tiles) for x in (sp, ap, cp, gp))
    sd = sd.reshape(SPAR, -1, LANES)
    groups = lax.axis_size("grp")
    kept = [(x.shape, x.dtype) for x in (w, ap, ph, kn, cp, ci, gp)]
    first, copies, w, ap, ph, kn, cp, ci, gp = call(
        attitude_kernel,
        [(tiles, F32), ((groups, 32, LANES), F32)] + kept,
        [vmem(x.shape, x.dtype) for x in (res, sp, si, sd)]
        + [
            vmem((60 * TILES, LANES), F32),
            vmem((LANES, rows), BF16),
            vmem((12 * TILES, LANES), F32),
            vmem((48, rows), BF16),
            vmem((LANES, rows), BF16),
            vmem((LANES // 2, LANES), F32),
            vmem((32, LANES), F32),
            pltpu.SemaphoreType.DMA((11,)),
        ],
        w, ap, ph, kn, cp, ci, gp, res, sp, si, sd, flops=1 << 24, far=True,
    )
    gathered = lax.all_to_all(copies, "grp", split_axis=0, concat_axis=0, tiled=True)
    zl, zr, hot = call(
        matrix_kernel,
        [((LO, LANES), F32), ((LO, LANES), F32), ((LO, rows), BF16)],
        [vmem((2, N_C * TILES, LANES), F32), vmem((2 * LANES, rows), BF16), vmem((2 * LANES, rows), BF16)],
        w, cp, ci, gp, kn, flops=1 << 27,
    )
    own = gathered.sum(axis=0)
    outside = paired(own, 1)
    inside = paired(own, 0)
    second, step, keep, send = call(
        sweep_kernel,
        [(tiles, F32), ((3, ND), F32), ((LO, LANES), F32), ((LO, LANES), F32)],
        [vmem((32, LANES), F32), vmem((3, CPAR * TILES, LANES), F32), vmem((3 * CPAR * HI, rows), BF16)],
        own, inside, outside, kn, first, ph, ap, w, cp, ci, gp, hot, zl, zr, flops=1 << 24,
    )
    z = (keep + paired(send, 0)).reshape(LO // 2, 2, LANES)
    z = lax.all_to_all(z, ("pair", "grp"), split_axis=0, concat_axis=0, tiled=True)
    copies, glob, glob_step = call(
        solve_kernel,
        [((LO, LANES), F32), ((2 * GPAR, LANES), F32), ((1, GPAR), F32)],
        [vmem((8, LANES), F32)],
        z.reshape(LO, LANES),
    )
    table = lax.all_to_all(copies.reshape(LO, 1, LANES), (*TM, "grp"), split_axis=0, concat_axis=0, tiled=True)
    out, calib = call(
        final_kernel,
        [(tiles, F32), ((CPAR, UNITS), F32)],
        [vmem((LANES, LO), F32)],
        table.reshape(LO, LANES), second, cp, ci, gp, glob,
    )
    return out.reshape(1, 1, rows), step, calib, glob_step.reshape(GPAR)


def solution(mesh):
    count, groups = mesh.devices.shape
    mesh = Mesh(mesh.devices.reshape(count // 2, 2, groups), (*TM, "grp"))
    return jax.shard_map(
        per_device,
        mesh=mesh,
        in_specs=(
            P(TM, "grp", None),
            P(TM, "grp", None),
            P(None, TM, "grp", None),
            P(TM, "grp", None),
            P(None, TM, None),
            P(None, TM, "grp", None),
            P(TM, "grp", None),
            P(TM, "grp", None),
            P(None, TM, "grp", None),
            P(TM, "grp", None),
            P(None, TM, "grp", None),
        ),
        out_specs=(P(TM, "grp", None), P(None, TM), P(), P()),
        check_vma=False,
    )
```
